256 devices in a mesh: space: 16 (over z, core), vel: 16 (over x, y).
Axes of the slice: x: 4, y: 4, z: 8, core: 2. Of those that a mesh axis runs over, the one named last changes fastest.
Arguments:
- distribution: float32 [1024, 32768], P('space', 'vel'), may hold values from 0.05 to 2
- collision_order: int32 [16, 64], P('space'), may hold values from 0 to 63, each once within a row
- collision_blocks: int32 [16], P('space'), may hold values from 1 to 4, 32 in all
- kernels: float32 [5, 32768], replicated, may hold values from -6 to 6
Outputs:
- new_distribution: float32 [1024, 32768], P('space', 'vel')
The draws below stay inside these ranges and needn't reach their ends.
Inputs may be any that keep to these rules, and one draw needn't show every extreme that they name: `collision_order`: each row is an ordering of the 64 local cells. `collision_blocks`: the counts sum to 32, which is 2 on average for each index of space, and the largest is 4.
All inputs are finite; a program needn't handle non-finite values. No bound on the sum of `collision_blocks` on one device may be relied on, other than what follows from the above.
Results may differ from the reference program's by a relative error of at most 0.0001.
Values sent between devices are 32-bit elements; how exact they have to be, the bound alone decides.
No kernel may reach another device: no remote copies, remote signals or barrier semaphores. Data moves between devices by JAX's collectives and lax.ppermute only.
A program may use at most 64 MiB of HBM per device.

```python
import math
import jax
import jax.numpy as jnp
import numpy as np
from jax import lax

NV = 32
QUAD = 2
BLOCK_CELLS = 16
CELLS_PER_RANK = 64
MAX_RANK_BLOCKS = 4
KERN = 5
VEL = 32768
CELLS = 1024
LISTED_BLOCKS = 32
N_SPACE = 16


def levels(stream_key, dims, cuts, smallest, largest):
    gain = 1.0
    for dim, parts in cuts:
        steps = jax.random.uniform(jax.random.fold_in(jax.random.fold_in(stream_key, 6), dim), (parts,), jnp.float32, smallest / len(cuts), largest / len(cuts))
        gain = gain * jnp.repeat(jnp.exp(steps), dims[dim] // parts).reshape((-1,) + (1,) * (len(dims) - 1 - dim))
    return gain


def profile(amount, total, reach, skew):
    portions = [(1 << 20) // math.isqrt(standing ** skew) + 1 for standing in range(2, amount + 1)]
    spare, holding = total - reach - (amount - 1), [1] * (amount - 1)
    while spare > 0:
        free = [i for i in range(amount - 1) if holding[i] < reach]
        whole, remaining = sum([portions[i] for i in free]), spare
        for i in free:
            addition = min(reach - holding[i], max(1, remaining * portions[i] // whole), spare)
            holding[i] = holding[i] + addition
            spare = spare - addition
    return np.array([reach] + holding)


def uneven_parts(stream_key, number_of, total, limit, skew):
    if number_of == 2:
        one = jax.random.randint(stream_key, (), max(1, total - limit), min(limit, total - 1) + 1)
        return jnp.stack([one, total - one])
    lengths = jnp.asarray(profile(number_of, total, limit, skew), jnp.int32)
    pairs = (number_of - 1) // 2
    source_of, taker = lengths[1:1 + 2 * pairs:2], lengths[2:2 + 2 * pairs:2]
    slack = jnp.minimum(source_of - 1, limit - taker)
    passed = jax.random.randint(jax.random.fold_in(stream_key, 1), (pairs,), 0, 1 << 20) % (slack + 1)
    lengths = lengths.at[1:1 + 2 * pairs:2].set(source_of - passed).at[2:2 + 2 * pairs:2].set(taker + passed)
    return lengths[jax.random.permutation(jax.random.fold_in(stream_key, 2), number_of)]


def bell_draw(rng, dims, width, reach, kind=jnp.bfloat16):
    return jnp.clip(width * jax.random.normal(rng, dims, jnp.float32), -reach, reach).astype(kind)


def setup_inputs(seed: int = 0) -> dict:
    arg_keys = jax.random.split(jax.random.key(seed), 5)
    distribution = jnp.clip(jnp.exp(math.log(2.0) - 3.6888794 * jax.random.uniform(arg_keys[0], (CELLS, VEL), jnp.float32) ** levels(arg_keys[0], (CELLS, VEL), ((0, 16), (1, 16)), -0.2, 0.2)), 0.05, 2.0)
    collision_order = jax.vmap(lambda own: jax.random.permutation(own, CELLS_PER_RANK))(jax.random.split(arg_keys[1], N_SPACE)).reshape((N_SPACE, CELLS_PER_RANK)).astype(jnp.int32)
    collision_blocks = uneven_parts(arg_keys[2], N_SPACE, LISTED_BLOCKS, MAX_RANK_BLOCKS, 2).astype(jnp.int32)
    kernels = bell_draw(arg_keys[3], (KERN, VEL), 1.0, 6.0, jnp.float32)
    return dict(distribution=distribution, collision_order=collision_order, collision_blocks=collision_blocks, kernels=kernels)


STEP_SCALE = 0.25
COURANT_MAX = 0.95


def courants(vel_width):
    vx_plane = (lax.iota(jnp.int32, vel_width) // (NV * NV)).astype(jnp.float32)
    courant = COURANT_MAX * (2.0 * vx_plane - (NV - 1)) / (NV - 1)
    return jnp.maximum(courant, 0.0), jnp.minimum(courant, 0.0)


def sweep(padded, upwind_pos, upwind_neg):
    centre = padded[1:-1]
    return centre - upwind_pos * (centre - padded[:-2]) - upwind_neg * (padded[2:] - centre)


def reference(distribution, collision_order, collision_blocks, kernels):
    upwind_pos, upwind_neg = courants(VEL)
    transported = distribution
    for sweep_turn in range(2):
        transported = sweep(jnp.pad(transported, ((1, 1), (0, 0))), upwind_pos, upwind_neg)
    cell_owner_rank = jnp.argsort(collision_order, axis=1).astype(jnp.int32)
    listed_flag = cell_owner_rank < (BLOCK_CELLS * collision_blocks)[:, None]
    weights = kernels.reshape(KERN, NV, NV, NV)

    def collide(cell_rows):
        velocity_cube = cell_rows.reshape(CELLS_PER_RANK, NV, NV, NV)
        spectrum = jnp.fft.fftn(velocity_cube, axes=(1, 2, 3))

        def inverse(weight):
            return jnp.real(jnp.fft.ifftn(spectrum * weight, axes=(1, 2, 3)))

        gain_term = jnp.zeros_like(velocity_cube)
        for quad_index in range(QUAD):
            gain_term = gain_term + inverse(weights[2 * quad_index]) * inverse(weights[2 * quad_index + 1])
        updated = velocity_cube + STEP_SCALE * (gain_term - velocity_cube * inverse(weights[2 * QUAD]))
        return updated.reshape(CELLS_PER_RANK, VEL)

    grouped = transported.reshape(N_SPACE, CELLS_PER_RANK, VEL)
    collided = lax.map(collide, grouped)
    return jnp.where(listed_flag[:, :, None], collided, grouped).reshape(CELLS, VEL)
```

```python
import functools
import math

import jax
import jax.numpy as jnp
import numpy as np
from jax import lax
from jax.experimental import pallas as pl
from jax.experimental.pallas import tpu as pltpu
from jax.sharding import Mesh
from jax.sharding import PartitionSpec as P

NV = 32
BLOCK_CELLS = 16
KERN = 5
VEL = ("vel_0", "vel_1")
COURANT_MAX = 0.95
STEP_SCALE = 0.25
F32 = jnp.float32
BF16 = jnp.bfloat16


def small_tables():
    lane = np.arange(128)
    y4, z = lane // 32, lane % 32
    base = (8 * np.outer(y4, y4) + np.outer(z, z)) % 32
    row = np.arange(512)
    v, x2, ch = row // 32, (row % 16) // 8, row % 8
    x = 2 * v + x2
    left = np.outer(np.arange(32), x) % 32
    turn = (4 * np.outer(np.arange(8), ch)) % 32
    tables = []
    for phase in (base, left, turn):
        angle = phase * (2.0 * math.pi / 32)
        tables += [np.cos(angle).astype(np.float32), np.sin(angle).astype(np.float32)]
    neg = (32 - z) % 32
    flips = []
    for other in ((4 - y4) % 4, 3 - y4):
        flip = np.zeros((128, 128), np.float32)
        flip[other * 32 + neg, lane] = 1.0
        flips.append(flip)
    tables.append(np.stack(flips))
    return tables


def split(a):
    hi = a.astype(BF16)
    lo = (a - hi.astype(F32)).astype(BF16)
    return hi, lo


def dot(a, b):
    return jnp.dot(a, b, preferred_element_type=F32)


def dot3(ahi, alo, bhi, blo):
    return dot(ahi, bhi) + dot(ahi, blo) + dot(alo, bhi)


def transport_kernel(side_ref, courant_ref, dist_ref, halo_ref, out_ref, raw):
    step = side_ref[0]
    zero = jnp.zeros((32, 128), F32)
    raw[0:32, :] = zero
    raw[66 * 16 : 68 * 16, :] = zero
    for tile in range(8):
        for j in range(16):
            raw[pl.ds((8 * tile + 2) * 16 + j, 8, stride=16), :] = dist_ref[
                8 * tile : 8 * tile + 8, 128 * j : 128 * j + 128
            ]
    at = pl.multiple_of(jnp.where(step < 0, 0, 66 * 16), 16)
    for j in range(16):
        raw[pl.ds(at + j, 2, stride=16), :] = halo_ref[:, 128 * j : 128 * j + 128]
    for cell in range(64):
        for half in range(2):
            a = courant_ref[half]
            here = (cell + 2) * 16 + 8 * half
            f0 = raw[pl.ds(here, 8), :]
            f1 = raw[pl.ds(pl.multiple_of(here + 16 * step, 8), 8), :]
            f2 = raw[pl.ds(pl.multiple_of(here + 32 * step, 8), 8), :]
            once = f0 - a * (f0 - f1)
            beside = f1 - a * (f1 - f2)
            out_ref[cell // 4, (cell % 4) * 16 + 8 * half : (cell % 4) * 16 + 8 * half + 8, :] = (
                once - a * (once - beside)
            )


def tables_kernel(
    where_ref, order_ref, kern_ref, c0_ref, s0_ref, cl_ref, sl_ref, ct_ref, st_ref, flip_ref,
    lhi_ref, llo_ref, ihi_ref, ilo_ref, whi_ref, wlo_ref, vhi_ref, vlo_ref, ks_ref, mask_ref,
    rows, turned, full,
):
    position = lax.broadcasted_iota(jnp.int32, (1, 64), 1)
    first = position < BLOCK_CELLS * where_ref[1]
    for c in range(4):
        hit = jnp.where(first & (order_ref[...] == 4 * where_ref[0] + c), STEP_SCALE, 0.0)
        mask_ref[16 * c : 16 * c + 16, :] = jnp.broadcast_to(
            jnp.sum(hit, axis=1, keepdims=True), (16, 128)
        )
    c0, s0 = c0_ref[...], s0_ref[...]
    lane_y4 = lax.broadcasted_iota(jnp.int32, (1, 128), 1) // 32
    for k8 in range(8):
        cosv = [math.cos(2 * math.pi * y4 * k8 / 32) for y4 in range(4)]
        sinv = [math.sin(2 * math.pi * y4 * k8 / 32) for y4 in range(4)]
        for y4 in range(4):
            part = slice(32 * y4, 32 * y4 + 32)
            lower = slice(128 + 32 * y4, 160 + 32 * y4)
            c = cosv[y4] * c0[part] - sinv[y4] * s0[part]
            s = cosv[y4] * s0[part] + sinv[y4] * c0[part]
            chi, clo = split(c)
            shi, slo = split(s)
            for ref, cc, ss in ((whi_ref, chi, shi), (wlo_ref, clo, slo)):
                ref[k8, part, 0:128] = cc
                ref[k8, part, 128:256] = -ss
                ref[k8, lower, 0:128] = ss
                ref[k8, lower, 128:256] = cc
        cvec = jnp.full((1, 128), cosv[0], F32)
        svec = jnp.full((1, 128), sinv[0], F32)
        for y4 in range(1, 4):
            cvec = jnp.where(lane_y4 == y4, cosv[y4], cvec)
            svec = jnp.where(lane_y4 == y4, sinv[y4], svec)
        c = cvec * c0 - svec * s0
        s = cvec * s0 + svec * c0
        chi, clo = split(c)
        shi, slo = split(s)
        for ref, cc, ss in ((vhi_ref, chi, shi), (vlo_ref, clo, slo)):
            ref[k8, 0:128, 0:128] = cc
            ref[k8, 0:128, 128:256] = ss
            ref[k8, 128:256, 0:128] = -ss
            ref[k8, 128:256, 128:256] = cc
    cl, sl = cl_ref[...], sl_ref[...]
    is_real = (lax.broadcasted_iota(jnp.int32, (1, 512), 1) // 16) % 2 == 0
    for k8 in range(8):
        ct, st = ct_ref[k8 : k8 + 1, :], st_ref[k8 : k8 + 1, :]
        c = ct * cl - st * sl
        s = ct * sl + st * cl
        full[64 * k8 : 64 * k8 + 32, :] = jnp.where(is_real, c, s)
        full[64 * k8 + 32 : 64 * k8 + 64, :] = jnp.where(is_real, -s, c)
    for i in range(4):
        part = slice(128 * i, 128 * i + 128)
        lhi_ref[part, :], llo_ref[part, :] = split(full[part, :])
        ihi_ref[part, :], ilo_ref[part, :] = split(full[:, part].T)
    for kx in range(32):
        for ch in range(8):
            at = kx * 8 + ch
            back = ((32 - kx) % 32) * 8 + ch
            tile = kern_ref[:, at * 128 : at * 128 + 128]
            rows[pl.ds(at, KERN, stride=256), :] = tile
            turned[pl.ds(back, KERN, stride=256), :] = tile
    group = lax.broadcasted_iota(jnp.int32, (32, 128), 1) // 32

    def ordered(src, t, k8):
        g, h = k8 % 4, k8 // 4
        out = None
        for k4 in range(4):
            piece = src[pl.ds(t * 256 + 2 * k4 + h, 32, stride=8), :]
            if k4 != g:
                piece = pltpu.roll(piece, ((k4 - g) % 4) * 32, 1)
            out = piece if out is None else jnp.where(group == k4, piece, out)
        return out

    scale = 0.5 / NV**3
    for k8 in range(8):
        flip = flip_ref[0 if k8 == 0 else 1].astype(BF16)
        for t in range(KERN):
            straight = ordered(rows, t, k8)
            other = ordered(turned, t, (8 - k8) % 8)
            hi, lo = split(other)
            mirrored = dot(hi, flip) + dot(lo, flip)
            ks_ref[k8, t] = scale * (straight + mirrored)


def collide_kernel(
    x_ref, lhi_ref, llo_ref, ihi_ref, ilo_ref, whi_ref, wlo_ref, vhi_ref, vlo_ref, ks_ref, mask_ref,
    out_ref, y, bhi, blo, acc,
):
    def cells(p):
        return x_ref[:, 32 * p : 32 * p + 32, :].reshape(512, 128)

    xhi, xlo = split(jnp.concatenate([cells(0), cells(1)], axis=1))
    y[...] = dot3(lhi_ref[...], llo_ref[...], xhi, xlo)
    for k8 in range(8):
        top = slice(64 * k8, 64 * k8 + 32)
        low = slice(64 * k8 + 32, 64 * k8 + 64)
        field = jnp.concatenate(
            [
                jnp.concatenate([y[top, 0:128], y[low, 0:128]], axis=1),
                jnp.concatenate([y[top, 128:256], y[low, 128:256]], axis=1),
            ],
            axis=0,
        )
        fhi, flo = split(field)
        spectrum = dot3(fhi, flo, whi_ref[k8], wlo_ref[k8])
        parts = []
        for t in range(KERN):
            ks = ks_ref[k8, t]
            ks = jnp.concatenate([ks, ks], axis=1)
            parts += [spectrum[0:32] * ks, spectrum[32:64] * ks]
        ghi, glo = split(jnp.concatenate(parts, axis=0))
        back = dot3(ghi, glo, vhi_ref[k8], vlo_ref[k8])
        hi, lo = split(back)
        for n in range(2 * KERN):
            for ref, val in ((bhi, hi), (blo, lo)):
                ref[top, 128 * n : 128 * n + 128] = val[32 * n : 32 * n + 32, 0:128]
                ref[low, 128 * n : 128 * n + 128] = val[32 * n : 32 * n + 32, 128:256]

    def part(t):
        cols = slice(256 * t, 256 * t + 256)
        return dot3(ihi_ref[...], ilo_ref[...], bhi[:, cols], blo[:, cols])

    acc[...] = part(0)
    acc[...] = acc[...] * part(1)
    y[...] = part(2)
    acc[...] = acc[...] + y[...] * part(3)
    y[...] = part(4)
    for p in range(2):
        lanes = slice(128 * p, 128 * p + 128)
        mask = mask_ref[32 * p : 32 * p + 32, :]
        for v in range(16):
            part_rows = slice(32 * v, 32 * v + 32)
            f = x_ref[v, 32 * p : 32 * p + 32, :]
            out_ref[v, 32 * p : 32 * p + 32, :] = f + mask * (
                acc[part_rows, lanes] - f * y[part_rows, lanes]
            )


def place_kernel(in_ref, out_ref):
    for tile in range(8):
        for j in range(16):
            out_ref[8 * tile : 8 * tile + 8, 128 * j : 128 * j + 128] = in_ref[
                pl.ds(tile * 128 + j, 8, stride=16), :
            ]


VM = pl.BlockSpec(memory_space=pltpu.VMEM)
SM = pl.BlockSpec(memory_space=pltpu.SMEM)


def shape(*dims, dtype=F32):
    return jax.ShapeDtypeStruct(dims, dtype)


def params(mib):
    return pltpu.CompilerParams(vmem_limit_bytes=mib << 20)


def transport(side, courant, dist, halo):
    return pl.pallas_call(
        transport_kernel,
        out_shape=shape(16, 64, 128),
        in_specs=[SM, SM, VM, VM],
        out_specs=VM,
        scratch_shapes=[pltpu.VMEM((68 * 16, 128), F32)],
        compiler_params=params(8),
        name="transport",
    )(side, courant, dist, halo)


def make_tables(where, order, kernels):
    tables = small_tables()
    half = shape(512, 512, dtype=BF16)
    eight = shape(8, 256, 256, dtype=BF16)
    return pl.pallas_call(
        tables_kernel,
        out_shape=[half] * 4 + [eight] * 4 + [shape(8, KERN, 32, 128), shape(64, 128)],
        in_specs=[SM] + [VM] * 9,
        out_specs=[VM] * 10,
        scratch_shapes=[
            pltpu.VMEM((KERN * 256, 128), F32),
            pltpu.VMEM((KERN * 256, 128), F32),
            pltpu.VMEM((512, 512), F32),
        ],
        compiler_params=params(20),
        name="tables",
    )(where, order, kernels, *[jnp.asarray(t) for t in tables])


def collide(x, tables):
    return pl.pallas_call(
        collide_kernel,
        out_shape=shape(16, 64, 128),
        in_specs=[VM] * 11,
        out_specs=VM,
        scratch_shapes=[
            pltpu.VMEM((512, 256), F32),
            pltpu.VMEM((512, 1280), BF16),
            pltpu.VMEM((512, 1280), BF16),
            pltpu.VMEM((512, 256), F32),
        ],
        compiler_params=params(24),
        name="collide",
    )(x, *tables)


def place(x):
    return pl.pallas_call(
        place_kernel,
        out_shape=shape(64, 2048),
        in_specs=[VM],
        out_specs=VM,
        compiler_params=params(8),
        name="place",
    )(x.reshape(1024, 128))


def local(distribution, collision_order, collision_blocks, kernels):
    v = lax.axis_index(VEL)
    rising = v >= 8
    x = 2 * v + lax.iota(jnp.int32, 2)
    courant = jnp.abs(COURANT_MAX * (2.0 * x.astype(F32) - (NV - 1)) / (NV - 1))
    side = jnp.where(rising, -1, 1).astype(jnp.int32)[None]
    edge = jnp.where(rising, distribution[62:64], distribution[0:2])
    pairs = []
    for s in range(16):
        for u in range(16):
            to = s + 1 if u >= 8 else s - 1
            if 0 <= to < 16:
                pairs.append((s * 16 + u, to * 16 + u))
    halo = lax.ppermute(edge, ("space",) + VEL, pairs)
    where = jnp.stack([v.astype(jnp.int32), collision_blocks[0]])
    tables = make_tables(where, collision_order, kernels)
    mine = transport(side, courant, distribution, halo)
    cells = lax.all_to_all(mine, VEL, split_axis=0, concat_axis=0, tiled=True)
    done = collide(cells, tables)
    back = lax.all_to_all(done, VEL, split_axis=0, concat_axis=0, tiled=True)
    return place(back)


def solution(mesh):
    finer = Mesh(mesh.devices.reshape(mesh.shape["space"], 4, 4), ("space", "vel_0", "vel_1"))
    in_specs = (P("space", VEL), P("space", None), P("space"), P())
    out_specs = P("space", VEL)
    return jax.shard_map(local, mesh=finer, in_specs=in_specs, out_specs=out_specs, check_vma=False)
```

```python
import math

import jax
import jax.numpy as jnp
import numpy as np
from jax import lax
from jax.experimental import pallas as pl
from jax.experimental.pallas import tpu as pltpu
from jax.sharding import Mesh
from jax.sharding import PartitionSpec as P

NV = 32
BLOCK_CELLS = 16
KERN = 5
VEL = ("vel_0", "vel_1")
COURANT_MAX = 0.95
STEP_SCALE = 0.25
F32 = jnp.float32
BF16 = jnp.bfloat16
SLOT = 64


def constant_rows():
    lane = np.arange(128)
    y4, z = lane // 32, lane % 32
    base = ((8 * np.outer(y4, y4) + np.outer(z, z)) % 32) * (2.0 * math.pi / 32)
    row = np.arange(32)
    x = 2 * (row % 16) + row // 16
    left = (np.outer(np.arange(32), x) % 32) * (2.0 * math.pi / 32)
    c, s = np.cos(left), np.sin(left)
    forward = np.block([[c, s], [-s, c]])
    neg = (32 - z) % 32
    flips = []
    for other in ((4 - y4) % 4, 3 - y4):
        flip = np.zeros((128, 128))
        flip[other * 32 + neg, lane] = 1.0
        flips.append(flip)
    both = np.concatenate([forward, forward.T], axis=1)
    return np.concatenate([np.cos(base), np.sin(base), both] + flips, axis=0).astype(np.float32)


def split(a):
    hi = a.astype(BF16)
    lo = (a - hi.astype(F32)).astype(BF16)
    return hi, lo


def dot(a, b):
    return jnp.dot(a, b, preferred_element_type=F32)


def upwind(f0, f1, f2, a):
    once = f0 - a * (f0 - f1)
    beside = f1 - a * (f1 - f2)
    return once - a * (once - beside)


def transport_kernel(side_ref, courant_ref, dist_ref, out_ref, edge_ref, raw):
    step = side_ref[0]
    zero = jnp.zeros((32, 128), F32)
    raw[0:32, :] = zero
    raw[66 * 16 : 68 * 16, :] = zero
    for tile in range(8):
        for j in range(16):
            raw[pl.ds((8 * tile + 2) * 16 + j, 8, stride=16), :] = dist_ref[
                8 * tile : 8 * tile + 8, 128 * j : 128 * j + 128
            ]
    for cell in range(64):
        for half in range(2):
            here = (cell + 2) * 16 + 8 * half
            f0 = raw[pl.ds(here, 8), :]
            f1 = raw[pl.ds(pl.multiple_of(here + 16 * step, 8), 8), :]
            f2 = raw[pl.ds(pl.multiple_of(here + 32 * step, 8), 8), :]
            out_ref[cell // 4, pl.ds(2 * (cell % 4) + half, 8, stride=8), :] = upwind(
                f0, f1, f2, courant_ref[half]
            )
    first = pl.multiple_of(jnp.where(step < 0, 32, 62 * 16), 16)
    edge_ref[...] = raw[pl.ds(first, SLOT), :]


def edge_kernel(side_ref, courant_ref, edge_ref, halo_ref, _, out_ref, raw, slot, sem):
    step = side_ref[0]
    raw[32:96, :] = edge_ref[...]
    at = pl.multiple_of(jnp.where(step < 0, 0, 96), 16)
    for j in range(16):
        raw[pl.ds(at + j, 2, stride=16), :] = halo_ref[:, 128 * j : 128 * j + 128]
    for cell in range(4):
        for half in range(2):
            here = (cell + 2) * 16 + 8 * half
            f0 = raw[pl.ds(here, 8), :]
            f1 = raw[pl.ds(pl.multiple_of(here + 16 * step, 8), 8), :]
            f2 = raw[pl.ds(pl.multiple_of(here + 32 * step, 8), 8), :]
            slot[pl.ds(2 * cell + half, 8, stride=8), :] = upwind(f0, f1, f2, courant_ref[half])
    copy = pltpu.make_async_copy(slot, out_ref.at[jnp.where(step < 0, 0, 15)], sem)
    copy.start()
    copy.wait()


def tables_kernel(
    where_ref, order_ref, kern_ref, const_ref, v_ref, left_ref, ks_ref, mask_ref, rows, turned
):
    position = lax.broadcasted_iota(jnp.int32, (1, 64), 1)
    first = position < BLOCK_CELLS * where_ref[1]
    for c in range(4):
        hit = jnp.where(first & (order_ref[...] == 4 * where_ref[0] + c), STEP_SCALE, 0.0)
        mask_ref[8 * c : 8 * c + 8, :] = jnp.broadcast_to(jnp.sum(hit, axis=1, keepdims=True), (8, 128))
    c0, s0 = const_ref[0:128, :], const_ref[128:256, :]
    lane_y4 = lax.broadcasted_iota(jnp.int32, (1, 128), 1) // 32
    for k8 in range(8):
        cvec, svec = turn(k8, lane_y4)
        for i, (cc, ss) in enumerate(
            zip(split(cvec * c0 - svec * s0), split(cvec * s0 + svec * c0))
        ):
            v_ref[k8, i, 0] = cc
            v_ref[k8, i, 1] = ss
    lhi, llo = split(const_ref[256:320, :])
    for i in range(2):
        part = slice(64 * i, 64 * i + 64)
        left_ref[i] = jnp.concatenate([lhi[:, part], lhi[:, part], llo[:, part]], axis=1)
    for kx in range(32):
        for ch in range(8):
            at = kx * 8 + ch
            back = ((32 - kx) % 32) * 8 + ch
            tile = kern_ref[:, at * 128 : at * 128 + 128]
            rows[pl.ds(at, KERN, stride=256), :] = tile
            turned[pl.ds(back, KERN, stride=256), :] = tile
    group = lax.broadcasted_iota(jnp.int32, (32, 128), 1) // 32

    def ordered(src, t, k8):
        g, h = k8 % 4, k8 // 4
        out = None
        for k4 in range(4):
            piece = src[pl.ds(t * 256 + 2 * k4 + h, 32, stride=8), :]
            if k4 != g:
                piece = pltpu.roll(piece, ((k4 - g) % 4) * 32, 1)
            out = piece if out is None else jnp.where(group == k4, piece, out)
        return out

    scale = 0.5 / NV**3
    for k8 in range(8):
        at = 320 if k8 == 0 else 448
        flip = const_ref[at : at + 128, :].astype(BF16)
        for t in range(KERN):
            straight = ordered(rows, t, k8)
            other = ordered(turned, t, (8 - k8) % 8)
            hi, lo = split(other)
            ks_ref[k8, t] = scale * (straight + (dot(hi, flip) + dot(lo, flip)))


def turn(k8, lane_y4):
    cvec = jnp.full((1, 128), 1.0, F32)
    svec = jnp.full((1, 128), 0.0, F32)
    for y4 in range(1, 4):
        angle = 2 * math.pi * y4 * k8 / 32
        cvec = jnp.where(lane_y4 == y4, math.cos(angle), cvec)
        svec = jnp.where(lane_y4 == y4, math.sin(angle), svec)
    return cvec, svec


def fft8(re, im):
    h = math.sqrt(0.5)
    ar = [re[j] + re[j + 4] for j in range(4)]
    ai = [im[j] + im[j + 4] for j in range(4)]
    dr = [re[j] - re[j + 4] for j in range(4)]
    di = [im[j] - im[j + 4] for j in range(4)]
    br = [dr[0], h * (dr[1] + di[1]), di[2], h * (di[3] - dr[3])]
    bi = [di[0], h * (di[1] - dr[1]), -dr[2], -h * (di[3] + dr[3])]
    outr, outi = [None] * 8, [None] * 8
    for odd, cr, ci in ((0, ar, ai), (1, br, bi)):
        s0r, s0i = cr[0] + cr[2], ci[0] + ci[2]
        s1r, s1i = cr[0] - cr[2], ci[0] - ci[2]
        s2r, s2i = cr[1] + cr[3], ci[1] + ci[3]
        s3r, s3i = ci[1] - ci[3], cr[3] - cr[1]
        outr[odd], outi[odd] = s0r + s2r, s0i + s2i
        outr[4 + odd], outi[4 + odd] = s0r - s2r, s0i - s2i
        outr[2 + odd], outi[2 + odd] = s1r + s3r, s1i + s3i
        outr[6 + odd], outi[6 + odd] = s1r - s3r, s1i - s3i
    return outr, outi


def right(v_ref, k8, i, inverse):
    c, s = v_ref[k8, i, 0], v_ref[k8, i, 1]
    up, down = (s, -s) if inverse else (-s, s)
    return jnp.concatenate(
        [jnp.concatenate([c, up], axis=1), jnp.concatenate([down, c], axis=1)], axis=0
    )


def collide_kernel(x_ref, v_ref, left_ref, ks_ref, mask_ref, out_ref, fwd, mid, back):
    for p in range(2):
        lanes = slice(128 * p, 128 * p + 128)
        for x2 in range(2):
            def cell_rows(ch, cell):
                at = 8 * ch + 2 * (2 * p + cell) + x2
                return x_ref[pl.ds(at, 16, stride=SLOT), :]

            re, im = fft8([cell_rows(ch, 0) for ch in range(8)], [cell_rows(ch, 1) for ch in range(8)])
            for k8 in range(8):
                for ri, val in ((0, re[k8]), (1, im[k8])):
                    hi, lo = split(val)
                    at = 32 * ri + 16 * x2
                    fwd[k8, at : at + 16, lanes] = hi
                    fwd[k8, 64 + at : 80 + at, lanes] = lo
                    fwd[k8, 128 + at : 144 + at, lanes] = hi
    lane_y4 = lax.broadcasted_iota(jnp.int32, (1, 128), 1) // 32
    whi, wlo = right(v_ref, 0, 0, False), right(v_ref, 0, 1, False)
    for k8 in range(8):
        y = dot(left_ref[0], fwd[k8])
        cvec, svec = turn(k8, lane_y4)
        fields = []
        for p in range(2):
            re, im = y[0:32, 128 * p : 128 * p + 128], y[32:64, 128 * p : 128 * p + 128]
            if k8:
                re, im = re * cvec + im * svec, im * cvec - re * svec
            fields.append(jnp.concatenate([re, im], axis=1))
        fhi, flo = split(jnp.concatenate(fields, axis=0))
        spectrum = dot(fhi, whi) + dot(flo, whi) + dot(fhi, wlo)
        parts = []
        for t in range(KERN):
            ks = ks_ref[k8, t]
            ks = jnp.concatenate([ks, ks], axis=1)
            parts += [spectrum[0:32] * ks, spectrum[32:64] * ks]
        ghi, glo = split(jnp.concatenate(parts, axis=0))
        vhi, vlo = right(v_ref, k8, 0, True), right(v_ref, k8, 1, True)
        hi, lo = split(dot(ghi, vhi) + dot(glo, vhi) + dot(ghi, vlo))
        for n in range(2 * KERN):
            lanes = slice(128 * n, 128 * n + 128)
            for ri in range(2):
                val = hi[32 * n : 32 * n + 32, 128 * ri : 128 * ri + 128]
                mid[32 * ri : 32 * ri + 32, lanes] = val
                mid[128 + 32 * ri : 160 + 32 * ri, lanes] = val
                mid[64 + 32 * ri : 96 + 32 * ri, lanes] = lo[
                    32 * n : 32 * n + 32, 128 * ri : 128 * ri + 128
                ]
        back[k8] = dot(left_ref[1], mid[...])
    for p in range(2):
        for x2 in range(2):
            for vh in range(2):
                def part(t):
                    lanes = slice(256 * t + 128 * p, 256 * t + 128 * p + 128)
                    at = 16 * x2 + 8 * vh
                    re = [back[k8, at : at + 8, lanes] for k8 in range(8)]
                    im = [back[k8, 32 + at : 40 + at, lanes] for k8 in range(8)]
                    im, re = fft8(im, re)
                    return re + im

                total = [a * b for a, b in zip(part(0), part(1))]
                second = part(2)
                total = [a + b * c for a, b, c in zip(total, second, part(3))]
                loss = part(4)
                for cell in range(2):
                    mask = mask_ref[8 * (2 * p + cell) : 8 * (2 * p + cell) + 8, :]
                    for ch in range(8):
                        at = vh * 8 * SLOT + 8 * ch + 2 * (2 * p + cell) + x2
                        f = x_ref[pl.ds(at, 8, stride=SLOT), :]
                        i = 8 * cell + ch
                        out_ref[pl.ds(at, 8, stride=SLOT), :] = f + mask * (total[i] - f * loss[i])


def place_kernel(in_ref, out_ref):
    for tile in range(8):
        for x2 in range(2):
            for ch in range(8):
                j = 8 * x2 + ch
                for k in range(2):
                    at = (2 * tile + k) * SLOT + 8 * ch + x2
                    out_ref[8 * tile + 4 * k : 8 * tile + 4 * k + 4, 128 * j : 128 * j + 128] = in_ref[
                        pl.ds(at, 4, stride=2), :
                    ]


VM = pl.BlockSpec(memory_space=pltpu.VMEM)
SM = pl.BlockSpec(memory_space=pltpu.SMEM)
ANY = pl.BlockSpec(memory_space=pl.ANY)


def shape(*dims, dtype=F32):
    return jax.ShapeDtypeStruct(dims, dtype)


def params(mib):
    return pltpu.CompilerParams(vmem_limit_bytes=mib << 20)


def transport(side, courant, dist):
    return pl.pallas_call(
        transport_kernel,
        out_shape=[shape(16, SLOT, 128), shape(SLOT, 128)],
        in_specs=[SM, SM, VM],
        out_specs=[VM, VM],
        scratch_shapes=[pltpu.VMEM((68 * 16, 128), F32)],
        compiler_params=params(8),
        cost_estimate=pl.CostEstimate(flops=4000000, bytes_accessed=1 << 20, transcendentals=0),
        name="transport",
    )(side, courant, dist)


def edges(side, courant, edge, halo, mine):
    return pl.pallas_call(
        edge_kernel,
        out_shape=shape(16, SLOT, 128),
        in_specs=[SM, SM, VM, VM, ANY],
        out_specs=ANY,
        input_output_aliases={4: 0},
        scratch_shapes=[
            pltpu.VMEM((128, 128), F32),
            pltpu.VMEM((SLOT, 128), F32),
            pltpu.SemaphoreType.DMA,
        ],
        compiler_params=params(8),
        name="edges",
    )(side, courant, edge, halo, mine)


def make_tables(where, order, kernels):
    return pl.pallas_call(
        tables_kernel,
        out_shape=[
            shape(8, 2, 2, 128, 128, dtype=BF16),
            shape(2, 64, 192, dtype=BF16),
            shape(8, KERN, 32, 128),
            shape(32, 128),
        ],
        in_specs=[SM] + [VM] * 3,
        out_specs=[VM] * 4,
        scratch_shapes=[pltpu.VMEM((KERN * 256, 128), F32), pltpu.VMEM((KERN * 256, 128), F32)],
        compiler_params=params(12),
        cost_estimate=pl.CostEstimate(flops=8000000, bytes_accessed=4 << 20, transcendentals=0),
        name="tables",
    )(where, order, kernels, jnp.asarray(constant_rows()))


def collide(x, tables):
    return pl.pallas_call(
        collide_kernel,
        out_shape=shape(16 * SLOT, 128),
        in_specs=[VM] * 5,
        out_specs=VM,
        scratch_shapes=[
            pltpu.VMEM((8, 192, 256), BF16),
            pltpu.VMEM((192, 1280), BF16),
            pltpu.VMEM((8, 64, 1280), F32),
        ],
        compiler_params=params(16),
        name="collide",
    )(x.reshape(16 * SLOT, 128), *tables).reshape(16, SLOT, 128)


def place(x):
    return pl.pallas_call(
        place_kernel,
        out_shape=shape(64, 2048),
        in_specs=[VM],
        out_specs=VM,
        compiler_params=params(8),
        name="place",
    )(x.reshape(16 * SLOT, 128))


def local(distribution, collision_order, collision_blocks, kernels):
    v = lax.axis_index(VEL)
    rising = v >= 8
    x = 2 * v + lax.iota(jnp.int32, 2)
    courant = jnp.abs(COURANT_MAX * (2.0 * x.astype(F32) - (NV - 1)) / (NV - 1))
    side = jnp.where(rising, -1, 1).astype(jnp.int32)[None]
    edge_rows = jnp.where(rising, distribution[62:64], distribution[0:2])
    pairs = []
    for s in range(16):
        for u in range(16):
            to = s + 1 if u >= 8 else s - 1
            if 0 <= to < 16:
                pairs.append((s * 16 + u, to * 16 + u))
    halo = lax.ppermute(edge_rows, ("space",) + VEL, pairs)
    mine, edge = transport(side, courant, distribution)
    mine = edges(side, courant, edge, halo, mine)
    where = jnp.stack([v.astype(jnp.int32), collision_blocks[0]])
    tables = make_tables(where, collision_order, kernels)
    cells = lax.all_to_all(mine, VEL, split_axis=0, concat_axis=0, tiled=True)
    done = collide(cells, tables)
    back = lax.all_to_all(done, VEL, split_axis=0, concat_axis=0, tiled=True)
    return place(back)


def solution(mesh):
    finer = Mesh(mesh.devices.reshape(mesh.shape["space"], 4, 4), ("space", "vel_0", "vel_1"))
    in_specs = (P("space", VEL), P("space", None), P("space"), P())
    out_specs = P("space", VEL)
    return jax.shard_map(local, mesh=finer, in_specs=in_specs, out_specs=out_specs, check_vma=False)
```

```python
import math

import jax
import jax.numpy as jnp
import numpy as np
from jax import lax
from jax.experimental import pallas as pl
from jax.experimental.pallas import tpu as pltpu
from jax.sharding import PartitionSpec as P

NV = 32
BLOCK_CELLS = 16
KERN = 5
COURANT_MAX = 0.95
STEP_SCALE = 0.25
F32 = jnp.float32
BF16 = jnp.bfloat16
SLOT = 64

THERE = (15, 14, 13, 12, 11, 10, 9, 8, 7, 6, 5, 4, 3, 2, 1, 0)
BACK = (15, 14, 13, 12, 11, 10, 9, 8, 7, 6, 5, 4, 3, 2, 1, 0)
THERE_AT = [THERE.index(v) for v in range(16)]
BACK_AT = [BACK.index(v) for v in range(16)]


def constant_rows():
    lane = np.arange(128)
    y4, z = lane // 32, lane % 32
    x = 2 * (lane // 8) + lane % 2
    unit = 2.0 * math.pi / 32
    parts = []
    for phase in (8 * np.outer(y4, y4) + np.outer(z, z), np.outer(np.arange(32), x), np.outer(x, z)):
        parts += [np.cos((phase % 32) * unit), np.sin((phase % 32) * unit)]
    neg = (32 - z) % 32
    for other in ((4 - y4) % 4, 3 - y4):
        flip = np.zeros((128, 128))
        flip[other * 32 + neg, lane] = 1.0
        parts.append(flip)
    return np.concatenate(parts, axis=0).astype(np.float32)


def split(a):
    hi = a.astype(BF16)
    lo = (a - hi.astype(F32)).astype(BF16)
    return hi, lo


def dot(a, b):
    return jnp.dot(a, b, preferred_element_type=F32)


def dot3(ahi, alo, bhi, blo):
    return dot(ahi, bhi) + dot(ahi, blo) + dot(alo, bhi)


def upwind(f0, f1, f2, a):
    once = f0 - a * (f0 - f1)
    beside = f1 - a * (f1 - f2)
    return once - a * (once - beside)


def sweeps(raw, cells, first, step, courant_ref, store):
    for cell in range(cells):
        for half in range(2):
            here = first + cell * 16 + 8 * half
            f0 = raw[pl.ds(here, 8), :]
            f1 = raw[pl.ds(pl.multiple_of(here + 16 * step, 8), 8), :]
            f2 = raw[pl.ds(pl.multiple_of(here + 32 * step, 8), 8), :]
            store(cell, half, upwind(f0, f1, f2, courant_ref[half]))


def transport_kernel(
    side_ref, courant_ref, dist_ref, out_ref, edge_ref, raw, slots, out_sem
):
    step = side_ref[0]
    zero = jnp.zeros((32, 128), F32)
    raw[0:32, :] = zero
    raw[66 * 16 : 68 * 16, :] = zero
    for tile in range(8):
        for j in range(16):
            raw[pl.ds((8 * tile + 2) * 16 + j, 8, stride=16), :] = dist_ref[
                8 * tile : 8 * tile + 8, 128 * j : 128 * j + 128
            ]
    stores = [
        pltpu.make_async_copy(slots.at[i], out_ref.at[i], out_sem.at[i]) for i in range(16)
    ]

    def store(cell, half, value):
        slots[THERE_AT[cell // 4], pl.ds(2 * (cell % 4) + half, 8, stride=8), :] = value
        if cell % 4 == 3 and half == 1:
            stores[THERE_AT[cell // 4]].start()

    sweeps(raw, 64, 32, step, courant_ref, store)
    edge_ref[...] = raw[pl.ds(pl.multiple_of(jnp.where(step < 0, 32, 62 * 16), 16), SLOT), :]
    for copy in stores:
        copy.wait()


def edge_kernel(side_ref, courant_ref, edge_ref, halo_ref, _, out_ref, raw, slot, sem):
    step = side_ref[0]
    raw[32:96, :] = edge_ref[...]
    at = pl.multiple_of(jnp.where(step < 0, 0, 96), 16)
    for j in range(16):
        raw[pl.ds(at + j, 2, stride=16), :] = halo_ref[:, 128 * j : 128 * j + 128]

    def store(cell, half, value):
        slot[pl.ds(2 * cell + half, 8, stride=8), :] = value

    sweeps(raw, 4, 32, step, courant_ref, store)
    copy = pltpu.make_async_copy(slot, out_ref.at[jnp.where(step < 0, THERE_AT[0], THERE_AT[15])], sem)
    copy.start()
    copy.wait()


def tables_kernel(
    where_ref, order_ref, kern_ref, const_ref, base_ref, ks_ref, mask_ref, rows, turned
):
    position = lax.broadcasted_iota(jnp.int32, (1, 64), 1)
    first = position < BLOCK_CELLS * where_ref[1]
    for c in range(4):
        hit = jnp.where(first & (order_ref[...] == 4 * where_ref[0] + c), STEP_SCALE, 0.0)
        mask_ref[2 * c : 2 * c + 2, :] = jnp.broadcast_to(jnp.sum(hit, axis=1, keepdims=True), (2, 128))
    base_ref[...] = const_ref[0:576, :]
    for kx in range(32):
        for ch in range(8):
            at = kx * 8 + ch
            back = ((32 - kx) % 32) * 8 + ch
            tile = kern_ref[:, at * 128 : at * 128 + 128]
            rows[pl.ds(at, KERN, stride=256), :] = tile
            turned[pl.ds(back, KERN, stride=256), :] = tile
    group = lax.broadcasted_iota(jnp.int32, (32, 128), 1) // 32

    def ordered(src, t, k8):
        g, h = k8 % 4, k8 // 4
        out = None
        for k4 in range(4):
            piece = src[pl.ds(t * 256 + 2 * k4 + h, 32, stride=8), :]
            if k4 != g:
                piece = pltpu.roll(piece, ((k4 - g) % 4) * 32, 1)
            out = piece if out is None else jnp.where(group == k4, piece, out)
        return out

    scale = 0.5 / NV**3
    for k8 in range(8):
        at = 576 if k8 == 0 else 704
        flip = const_ref[at : at + 128, :].astype(BF16)
        for t in range(KERN):
            straight = ordered(rows, t, k8)
            other = ordered(turned, t, (8 - k8) % 8)
            hi, lo = split(other)
            ks_ref[k8, t] = scale * (straight + (dot(hi, flip) + dot(lo, flip)))


def turn(k8, lane_y4):
    cvec = jnp.full((1, 128), 1.0, F32)
    svec = jnp.full((1, 128), 0.0, F32)
    for y4 in range(1, 4):
        angle = 2 * math.pi * y4 * k8 / 32
        cvec = jnp.where(lane_y4 == y4, math.cos(angle), cvec)
        svec = jnp.where(lane_y4 == y4, math.sin(angle), svec)
    return cvec, svec


ROOT = math.sqrt(0.5)
PAIRS = ((0, 4), (1, 7), (2, 6), (3, 5))


def forward8(x):
    a = [x[j] + x[j + 4] for j in range(4)]
    d = [x[j] - x[j + 4] for j in range(4)]
    even, odd = a[0] + a[2], a[1] + a[3]
    less, more = ROOT * (d[1] - d[3]), ROOT * (d[1] + d[3])
    return (
        (even + odd, even - odd),
        (d[0] + less, -d[2] - more),
        (a[0] - a[2], a[3] - a[1]),
        (d[0] - less, d[2] - more),
    )


def inverse8(r0, r4, c1, s1, c2, s2, c3, s3):
    e, o = r0 + r4, r0 - r4
    a, b, c, d = e + c2, e - c2, c1 + c3, s3 - s1
    p, q = o - s2, o + s2
    less, more = ROOT * (c1 - c3), ROOT * (s1 + s3)
    m, n = less - more, less + more
    return [a + c, p + m, b + d, q - n, a - c, p - m, b - d, q + n]


def right(base_ref, k8, inverse):
    c, s = base_ref[0:128, :], base_ref[128:256, :]
    if k8:
        cvec, svec = turn(k8, lax.broadcasted_iota(jnp.int32, (1, 128), 1) // 32)
        c, s = cvec * c - svec * s, cvec * s + svec * c
    halves = []
    for c, s in zip(split(c), split(s)):
        up, down = (s, -s) if inverse else (-s, s)
        halves.append(
            jnp.concatenate(
                [jnp.concatenate([c, up], axis=1), jnp.concatenate([down, c], axis=1)], axis=0
            )
        )
    return halves


def left_matrices(base_ref, lf_ref, li_ref):
    zero = jnp.zeros((32, 128), BF16)
    c, s = base_ref[256:288, :], base_ref[288:320, :]
    cell = (lax.broadcasted_iota(jnp.int32, (32, 128), 1) % 8) // 2
    for p in range(2):
        first, second = cell == 2 * p, cell == 2 * p + 1
        real = split(jnp.where(first, c, jnp.where(second, s, 0.0)))
        imag = split(jnp.where(first, -s, jnp.where(second, c, 0.0)))
        for half in range(2):
            re, im = real[half], imag[half]
            for kk in range(2):
                at = 128 * kk + 64 * p
                top, low = slice(at, at + 32), slice(at + 32, at + 64)
                mine, other = slice(128 * kk, 128 * kk + 128), slice(128 - 128 * kk, 256 - 128 * kk)
                lf_ref[0, half, top, mine], lf_ref[0, half, low, mine] = re, im
                lf_ref[0, half, top, other], lf_ref[0, half, low, other] = zero, zero
                lf_ref[1, half, top, 0:128], lf_ref[1, half, low, 0:128] = re, im
                lf_ref[1, half, top, 128:256] = im if kk else -im
                lf_ref[1, half, low, 128:256] = -re if kk else re
    zero = jnp.zeros((128, 128), BF16)
    c, s = base_ref[320:448, :], base_ref[448:576, :]
    cell = (lax.broadcasted_iota(jnp.int32, (128, 128), 0) % 8) // 2
    lane = lax.broadcasted_iota(jnp.int32, (128, 128), 1)
    first, second = cell == 2 * (lane // 64), cell == 2 * (lane // 64) + 1
    real = (lane // 32) % 2 == 0
    zeroth = split(jnp.where(first, jnp.where(real, c, -s), jnp.where(second, jnp.where(real, s, c), 0.0)))
    other = split(jnp.where(first, jnp.where(real, s, c), jnp.where(second, jnp.where(real, -c, s), 0.0)))
    for half in range(2):
        a, b = zeroth[half], other[half]
        up, low = slice(0, 128), slice(128, 256)
        li_ref[0, half, up, up], li_ref[0, half, up, low] = a, zero
        li_ref[0, half, low, up], li_ref[0, half, low, low] = zero, a
        li_ref[1, half, up, up], li_ref[1, half, up, low] = a, a
        li_ref[1, half, low, up], li_ref[1, half, low, low] = b, -b


def collide_kernel(
    x_ref, base_ref, ks_ref, mask_ref, out_ref, lf_ref, li_ref, fh, fl, y, gh, gl, spec, mh, ml, back
):
    left_matrices(base_ref, lf_ref, li_ref)
    for v in range(0, 16, 2):
        x = [
            jnp.concatenate(
                [x_ref[THERE_AT[v + i], 8 * ch : 8 * ch + 8, :] for i in range(2)], axis=0
            )
            for ch in range(8)
        ]
        for g, parts in enumerate(forward8(x)):
            for u, part in enumerate(parts):
                rows, lanes = slice(128 * u + 8 * v, 128 * u + 8 * v + 16), slice(128 * g, 128 * g + 128)
                fh[rows, lanes], fl[rows, lanes] = split(part)
    for i, lanes in enumerate((slice(0, 128), slice(128, 512))):
        y[:, lanes] = dot3(lf_ref[i, 0], lf_ref[i, 1], fh[:, lanes], fl[:, lanes])
    lane_y4 = lax.broadcasted_iota(jnp.int32, (1, 128), 1) // 32
    for g in range(4):
        for kk in range(2):
            k8 = PAIRS[g][kk]
            cvec, svec = turn(k8, lane_y4)
            for p in range(2):
                at = 128 * kk + 64 * p
                lanes = slice(128 * g, 128 * g + 128)
                re, im = y[at : at + 32, lanes], y[at + 32 : at + 64, lanes]
                if k8:
                    re, im = re * cvec + im * svec, im * cvec - re * svec
                rows = slice(64 * k8 + 32 * p, 64 * k8 + 32 * p + 32)
                gh[rows, 0:128], gl[rows, 0:128] = split(re)
                gh[rows, 128:256], gl[rows, 128:256] = split(im)
    spec[...] = dot3(gh[...], gl[...], *right(base_ref, 0, False))
    for g in range(4):
        for kk in range(2):
            k8 = PAIRS[g][kk]
            parts = []
            for t in range(KERN):
                ks = ks_ref[k8, t]
                ks = jnp.concatenate([ks, ks], axis=1)
                for p in range(2):
                    at = 64 * k8 + 32 * p
                    parts.append(spec[at : at + 32, :] * ks)
            hi, lo = split(jnp.concatenate(parts, axis=0))
            done = dot3(hi, lo, *right(base_ref, k8, True))
            hi, lo = split(done)
            for n in range(2 * KERN):
                t, p = n // 2, n % 2
                lanes = slice(128 * (KERN * g + t), 128 * (KERN * g + t) + 128)
                for ri in range(2):
                    at = 128 * kk + 64 * p + 32 * ri
                    part = (slice(32 * n, 32 * n + 32), slice(128 * ri, 128 * ri + 128))
                    mh[at : at + 32, lanes] = hi[part]
                    ml[at : at + 32, lanes] = lo[part]
    for i, lanes in enumerate((slice(0, 640), slice(640, 2560))):
        back[:, lanes] = dot3(li_ref[i, 0], li_ref[i, 1], mh[:, lanes], ml[:, lanes])
    mask = mask_ref[...]
    for v in range(16):
        def part(t):
            parts = []
            for g in range(4):
                lanes = slice(128 * (KERN * g + t), 128 * (KERN * g + t) + 128)
                for u in range(2):
                    parts.append(back[128 * u + 8 * v : 128 * u + 8 * v + 8, lanes])
            return inverse8(*parts)

        total = [a * b for a, b in zip(part(0), part(1))]
        total = [a + b * c for a, b, c in zip(total, part(2), part(3))]
        for ch, (gain, loss) in enumerate(zip(total, part(4))):
            f = x_ref[THERE_AT[v], 8 * ch : 8 * ch + 8, :]
            out_ref[BACK_AT[v], 8 * ch : 8 * ch + 8, :] = f + mask * (gain - f * loss)


def place_kernel(in_ref, out_ref, out, sem):
    stores = [
        pltpu.make_async_copy(out.at[pl.ds(8 * i, 8)], out_ref.at[pl.ds(8 * i, 8)], sem.at[i])
        for i in range(8)
    ]
    for tile in range(8):
        for x2 in range(2):
            for ch in range(8):
                j = 8 * x2 + ch
                for k in range(2):
                    at = BACK_AT[2 * tile + k] * SLOT + 8 * ch + x2
                    out[8 * tile + 4 * k : 8 * tile + 4 * k + 4, 128 * j : 128 * j + 128] = in_ref[
                        pl.ds(at, 4, stride=2), :
                    ]
        stores[tile].start()
    for copy in stores:
        copy.wait()


VM = pl.BlockSpec(memory_space=pltpu.VMEM)
SM = pl.BlockSpec(memory_space=pltpu.SMEM)
ANY = pl.BlockSpec(memory_space=pl.ANY)


def shape(*dims, dtype=F32):
    return jax.ShapeDtypeStruct(dims, dtype)


def params(mib):
    return pltpu.CompilerParams(vmem_limit_bytes=mib << 20)


def transport(side, courant, dist):
    return pl.pallas_call(
        transport_kernel,
        out_shape=[shape(16, SLOT, 128), shape(SLOT, 128)],
        in_specs=[SM, SM, VM],
        out_specs=[ANY, VM],
        scratch_shapes=[
            pltpu.VMEM((68 * 16, 128), F32),
            pltpu.VMEM((16, SLOT, 128), F32),
            pltpu.SemaphoreType.DMA((16,)),
        ],
        compiler_params=params(8),
        cost_estimate=pl.CostEstimate(flops=4000000, bytes_accessed=1 << 20, transcendentals=0),
        name="transport",
    )(side, courant, dist)


def edges(side, courant, edge, halo, mine):
    return pl.pallas_call(
        edge_kernel,
        out_shape=shape(16, SLOT, 128),
        in_specs=[SM, SM, VM, VM, ANY],
        out_specs=ANY,
        input_output_aliases={4: 0},
        scratch_shapes=[
            pltpu.VMEM((128, 128), F32),
            pltpu.VMEM((SLOT, 128), F32),
            pltpu.SemaphoreType.DMA,
        ],
        compiler_params=params(8),
        name="edges",
    )(side, courant, edge, halo, mine)


def make_tables(where, order, kernels):
    rows = pltpu.VMEM((KERN * 256, 128), F32)
    return pl.pallas_call(
        tables_kernel,
        out_shape=[shape(576, 128), shape(8, KERN, 32, 128), shape(8, 128)],
        in_specs=[SM] + [VM] * 3,
        out_specs=[VM] * 3,
        scratch_shapes=[rows, rows],
        compiler_params=params(12),
        cost_estimate=pl.CostEstimate(flops=8000000, bytes_accessed=4 << 20, transcendentals=0),
        name="tables",
    )(where, order, kernels, jnp.asarray(constant_rows()))


def collide(x, tables):
    left = pltpu.VMEM((2, 2, 256, 256), BF16)
    half = pltpu.VMEM((256, 512), BF16)
    field = pltpu.VMEM((512, 256), BF16)
    wide = pltpu.VMEM((256, 2560), BF16)
    return pl.pallas_call(
        collide_kernel,
        out_shape=shape(16, SLOT, 128),
        in_specs=[VM] * 4,
        out_specs=VM,
        scratch_shapes=[
            left,
            left,
            half,
            half,
            pltpu.VMEM((256, 512), F32),
            field,
            field,
            pltpu.VMEM((512, 256), F32),
            wide,
            wide,
            pltpu.VMEM((256, 2560), F32),
        ],
        compiler_params=params(20),
        name="collide",
    )(x, *tables)


def place(x):
    return pl.pallas_call(
        place_kernel,
        out_shape=shape(64, 2048),
        in_specs=[VM],
        out_specs=ANY,
        scratch_shapes=[pltpu.VMEM((64, 2048), F32), pltpu.SemaphoreType.DMA((8,))],
        compiler_params=params(8),
        name="place",
    )(x.reshape(16 * SLOT, 128))


def exchange(slots, order):
    return lax.all_to_all(
        slots, "vel", split_axis=0, concat_axis=0, tiled=True, axis_index_groups=[list(order)]
    )


def local(distribution, collision_order, collision_blocks, kernels):
    v = lax.axis_index("vel")
    rising = v >= 8
    x = 2 * v + lax.iota(jnp.int32, 2)
    courant = jnp.abs(COURANT_MAX * (2.0 * x.astype(F32) - (NV - 1)) / (NV - 1))
    side = jnp.where(rising, -1, 1).astype(jnp.int32)[None]
    pairs = []
    for s in range(16):
        for u in range(16):
            to = s + 1 if u >= 8 else s - 1
            if 0 <= to < 16:
                pairs.append((s * 16 + u, to * 16 + u))
    send = jnp.where(rising, distribution[62:64], distribution[0:2])
    mine, edge = transport(side, courant, distribution)
    halo = lax.ppermute(send, ("space", "vel"), pairs)
    mine = edges(side, courant, edge, halo, mine)
    where = jnp.stack([v.astype(jnp.int32), collision_blocks[0]])
    tables = make_tables(where, collision_order, kernels)
    cells = exchange(mine, THERE)
    return place(exchange(collide(cells, tables), BACK))


def solution(mesh):
    in_specs = (P("space", "vel"), P("space", None), P("space"), P())
    out_specs = P("space", "vel")
    return jax.shard_map(local, mesh=mesh, in_specs=in_specs, out_specs=out_specs, check_vma=False)
```

```python
import math

import jax
import jax.numpy as jnp
import numpy as np
from jax import lax
from jax.experimental import pallas as pl
from jax.experimental.pallas import tpu as pltpu
from jax.sharding import PartitionSpec as P

NV = 32
BLOCK_CELLS = 16
KERN = 5
COURANT_MAX = 0.95
STEP_SCALE = 0.25
F32 = jnp.float32
BF16 = jnp.bfloat16
SLOT = 64

THERE = (10, 11, 14, 15, 9, 13, 6, 7, 5, 8, 12, 2, 3, 1, 4, 0)
BACK = (10, 15, 5, 0, 11, 14, 4, 1, 9, 12, 6, 3, 8, 13, 7, 2)
THERE_AT = [THERE.index(v) for v in range(16)]
BACK_AT = [BACK.index(v) for v in range(16)]


def constant_rows():
    lane = np.arange(128)
    y4, z = lane // 32, lane % 32
    x = 2 * (lane // 8) + lane % 2
    unit = 2.0 * math.pi / 32
    parts = []
    for phase in (8 * np.outer(y4, y4) + np.outer(z, z), np.outer(np.arange(32), x), np.outer(x, z)):
        parts += [np.cos((phase % 32) * unit), np.sin((phase % 32) * unit)]
    neg = (32 - z) % 32
    for other in ((4 - y4) % 4, 3 - y4):
        flip = np.zeros((128, 128))
        flip[other * 32 + neg, lane] = 1.0
        parts.append(flip)
    return np.concatenate(parts, axis=0).astype(np.float32)


def split(a):
    hi = a.astype(BF16)
    lo = (a - hi.astype(F32)).astype(BF16)
    return hi, lo


def dot(a, b):
    return jnp.dot(a, b, preferred_element_type=F32)


def dot3(ahi, alo, bhi, blo):
    return dot(ahi, bhi) + dot(ahi, blo) + dot(alo, bhi)


def upwind(f0, f1, f2, a):
    once = f0 - a * (f0 - f1)
    beside = f1 - a * (f1 - f2)
    return once - a * (once - beside)


def sweeps(raw, cells, first, step, courant_ref, store):
    for cell in range(cells):
        for half in range(2):
            here = first + cell * 16 + 8 * half
            f0 = raw[pl.ds(here, 8), :]
            f1 = raw[pl.ds(pl.multiple_of(here + 16 * step, 8), 8), :]
            f2 = raw[pl.ds(pl.multiple_of(here + 32 * step, 8), 8), :]
            store(cell, half, upwind(f0, f1, f2, courant_ref[half]))


def transport_kernel(
    side_ref, courant_ref, dist_ref, out_ref, edge_ref, raw, slots, out_sem
):
    step = side_ref[0]
    zero = jnp.zeros((32, 128), F32)
    raw[0:32, :] = zero
    raw[66 * 16 : 68 * 16, :] = zero
    for tile in range(8):
        for j in range(16):
            raw[pl.ds((8 * tile + 2) * 16 + j, 8, stride=16), :] = dist_ref[
                8 * tile : 8 * tile + 8, 128 * j : 128 * j + 128
            ]
    stores = [
        pltpu.make_async_copy(slots.at[i], out_ref.at[i], out_sem.at[i]) for i in range(16)
    ]

    def store(cell, half, value):
        slots[THERE_AT[cell // 4], pl.ds(2 * (cell % 4) + half, 8, stride=8), :] = value
        if cell % 4 == 3 and half == 1:
            stores[THERE_AT[cell // 4]].start()

    sweeps(raw, 64, 32, step, courant_ref, store)
    edge_ref[...] = raw[pl.ds(pl.multiple_of(jnp.where(step < 0, 32, 62 * 16), 16), SLOT), :]
    for copy in stores:
        copy.wait()


def edge_kernel(side_ref, courant_ref, edge_ref, halo_ref, _, out_ref, raw, slot, sem):
    step = side_ref[0]
    raw[32:96, :] = edge_ref[...]
    at = pl.multiple_of(jnp.where(step < 0, 0, 96), 16)
    for j in range(16):
        raw[pl.ds(at + j, 2, stride=16), :] = halo_ref[:, 128 * j : 128 * j + 128]

    def store(cell, half, value):
        slot[pl.ds(2 * cell + half, 8, stride=8), :] = value

    sweeps(raw, 4, 32, step, courant_ref, store)
    copy = pltpu.make_async_copy(slot, out_ref.at[jnp.where(step < 0, THERE_AT[0], THERE_AT[15])], sem)
    copy.start()
    copy.wait()


def tables_kernel(
    where_ref, order_ref, kern_ref, const_ref, base_ref, ks_ref, mask_ref, rows, turned
):
    position = lax.broadcasted_iota(jnp.int32, (1, 64), 1)
    first = position < BLOCK_CELLS * where_ref[1]
    for c in range(4):
        hit = jnp.where(first & (order_ref[...] == 4 * where_ref[0] + c), STEP_SCALE, 0.0)
        mask_ref[2 * c : 2 * c + 2, :] = jnp.broadcast_to(jnp.sum(hit, axis=1, keepdims=True), (2, 128))
    base_ref[...] = const_ref[0:576, :]
    for kx in range(32):
        for ch in range(8):
            at = kx * 8 + ch
            back = ((32 - kx) % 32) * 8 + ch
            tile = kern_ref[:, at * 128 : at * 128 + 128]
            rows[pl.ds(at, KERN, stride=256), :] = tile
            turned[pl.ds(back, KERN, stride=256), :] = tile
    group = lax.broadcasted_iota(jnp.int32, (32, 128), 1) // 32

    def ordered(src, t, k8):
        g, h = k8 % 4, k8 // 4
        out = None
        for k4 in range(4):
            piece = src[pl.ds(t * 256 + 2 * k4 + h, 32, stride=8), :]
            if k4 != g:
                piece = pltpu.roll(piece, ((k4 - g) % 4) * 32, 1)
            out = piece if out is None else jnp.where(group == k4, piece, out)
        return out

    scale = 0.5 / NV**3
    for k8 in range(8):
        at = 576 if k8 == 0 else 704
        flip = const_ref[at : at + 128, :].astype(BF16)
        for t in range(KERN):
            straight = ordered(rows, t, k8)
            other = ordered(turned, t, (8 - k8) % 8)
            hi, lo = split(other)
            ks_ref[k8, t] = scale * (straight + (dot(hi, flip) + dot(lo, flip)))


def turn(k8, lane_y4):
    cvec = jnp.full((1, 128), 1.0, F32)
    svec = jnp.full((1, 128), 0.0, F32)
    for y4 in range(1, 4):
        angle = 2 * math.pi * y4 * k8 / 32
        cvec = jnp.where(lane_y4 == y4, math.cos(angle), cvec)
        svec = jnp.where(lane_y4 == y4, math.sin(angle), svec)
    return cvec, svec


ROOT = math.sqrt(0.5)
PAIRS = ((0, 4), (1, 7), (2, 6), (3, 5))


def forward8(x):
    a = [x[j] + x[j + 4] for j in range(4)]
    d = [x[j] - x[j + 4] for j in range(4)]
    even, odd = a[0] + a[2], a[1] + a[3]
    less, more = ROOT * (d[1] - d[3]), ROOT * (d[1] + d[3])
    return (
        (even + odd, even - odd),
        (d[0] + less, -d[2] - more),
        (a[0] - a[2], a[3] - a[1]),
        (d[0] - less, d[2] - more),
    )


def inverse8(r0, r4, c1, s1, c2, s2, c3, s3):
    e, o = r0 + r4, r0 - r4
    a, b, c, d = e + c2, e - c2, c1 + c3, s3 - s1
    p, q = o - s2, o + s2
    less, more = ROOT * (c1 - c3), ROOT * (s1 + s3)
    m, n = less - more, less + more
    return [a + c, p + m, b + d, q - n, a - c, p - m, b - d, q + n]


def right(base_ref, k8, inverse):
    c, s = base_ref[0:128, :], base_ref[128:256, :]
    if k8:
        cvec, svec = turn(k8, lax.broadcasted_iota(jnp.int32, (1, 128), 1) // 32)
        c, s = cvec * c - svec * s, cvec * s + svec * c
    halves = []
    for c, s in zip(split(c), split(s)):
        up, down = (s, -s) if inverse else (-s, s)
        halves.append(
            jnp.concatenate(
                [jnp.concatenate([c, up], axis=1), jnp.concatenate([down, c], axis=1)], axis=0
            )
        )
    return halves


def left_matrices(base_ref, lf_ref, li_ref):
    zero = jnp.zeros((32, 128), BF16)
    c, s = base_ref[256:288, :], base_ref[288:320, :]
    cell = (lax.broadcasted_iota(jnp.int32, (32, 128), 1) % 8) // 2
    for p in range(2):
        first, second = cell == 2 * p, cell == 2 * p + 1
        real = split(jnp.where(first, c, jnp.where(second, s, 0.0)))
        imag = split(jnp.where(first, -s, jnp.where(second, c, 0.0)))
        for half in range(2):
            re, im = real[half], imag[half]
            for kk in range(2):
                at = 128 * kk + 64 * p
                top, low = slice(at, at + 32), slice(at + 32, at + 64)
                mine, other = slice(128 * kk, 128 * kk + 128), slice(128 - 128 * kk, 256 - 128 * kk)
                lf_ref[0, half, top, mine], lf_ref[0, half, low, mine] = re, im
                lf_ref[0, half, top, other], lf_ref[0, half, low, other] = zero, zero
                lf_ref[1, half, top, 0:128], lf_ref[1, half, low, 0:128] = re, im
                lf_ref[1, half, top, 128:256] = im if kk else -im
                lf_ref[1, half, low, 128:256] = -re if kk else re
    zero = jnp.zeros((128, 128), BF16)
    c, s = base_ref[320:448, :], base_ref[448:576, :]
    cell = (lax.broadcasted_iota(jnp.int32, (128, 128), 0) % 8) // 2
    lane = lax.broadcasted_iota(jnp.int32, (128, 128), 1)
    first, second = cell == 2 * (lane // 64), cell == 2 * (lane // 64) + 1
    real = (lane // 32) % 2 == 0
    zeroth = split(jnp.where(first, jnp.where(real, c, -s), jnp.where(second, jnp.where(real, s, c), 0.0)))
    other = split(jnp.where(first, jnp.where(real, s, c), jnp.where(second, jnp.where(real, -c, s), 0.0)))
    for half in range(2):
        a, b = zeroth[half], other[half]
        up, low = slice(0, 128), slice(128, 256)
        li_ref[0, half, up, up], li_ref[0, half, up, low] = a, zero
        li_ref[0, half, low, up], li_ref[0, half, low, low] = zero, a
        li_ref[1, half, up, up], li_ref[1, half, up, low] = a, a
        li_ref[1, half, low, up], li_ref[1, half, low, low] = b, -b


def columns(g, t):
    at = 128 * (t if g == 0 else KERN + 3 * t + g - 1)
    return slice(at, at + 128)


def collide_kernel(
    x_ref, base_ref, ks_ref, mask_ref, out_ref, lf_ref, li_ref, fh, fl, y, gh, gl, spec, mh, ml, back, total
):
    left_matrices(base_ref, lf_ref, li_ref)
    for v in range(0, 16, 2):
        x = [
            jnp.concatenate(
                [x_ref[THERE_AT[v + i], 8 * ch : 8 * ch + 8, :] for i in range(2)], axis=0
            )
            for ch in range(8)
        ]
        for g, parts in enumerate(forward8(x)):
            for u, part in enumerate(parts):
                rows, lanes = slice(128 * u + 8 * v, 128 * u + 8 * v + 16), slice(128 * g, 128 * g + 128)
                fh[rows, lanes], fl[rows, lanes] = split(part)
    for i, lanes in enumerate((slice(0, 128), slice(128, 512))):
        y[:, lanes] = dot3(lf_ref[i, 0], lf_ref[i, 1], fh[:, lanes], fl[:, lanes])
    lane_y4 = lax.broadcasted_iota(jnp.int32, (1, 128), 1) // 32
    for g in range(4):
        for kk in range(2):
            k8 = PAIRS[g][kk]
            cvec, svec = turn(k8, lane_y4)
            for p in range(2):
                at = 128 * kk + 64 * p
                lanes = slice(128 * g, 128 * g + 128)
                re, im = y[at : at + 32, lanes], y[at + 32 : at + 64, lanes]
                if k8:
                    re, im = re * cvec + im * svec, im * cvec - re * svec
                rows = slice(64 * k8 + 32 * p, 64 * k8 + 32 * p + 32)
                gh[rows, 0:128], gl[rows, 0:128] = split(re)
                gh[rows, 128:256], gl[rows, 128:256] = split(im)
    spec[...] = dot3(gh[...], gl[...], *right(base_ref, 0, False))
    for g in range(4):
        for kk in range(2):
            k8 = PAIRS[g][kk]
            parts = []
            for t in range(KERN):
                ks = ks_ref[k8, t]
                ks = jnp.concatenate([ks, ks], axis=1)
                for p in range(2):
                    at = 64 * k8 + 32 * p
                    parts.append(spec[at : at + 32, :] * ks)
            hi, lo = split(jnp.concatenate(parts, axis=0))
            done = dot3(hi, lo, *right(base_ref, k8, True))
            hi, lo = split(done)
            for n in range(2 * KERN):
                t, p = n // 2, n % 2
                for ri in range(2):
                    at = 128 * kk + 64 * p + 32 * ri
                    part = (slice(32 * n, 32 * n + 32), slice(128 * ri, 128 * ri + 128))
                    mh[at : at + 32, columns(g, t)] = hi[part]
                    ml[at : at + 32, columns(g, t)] = lo[part]

    def over_x(i, lanes):
        back[:, lanes] = dot3(li_ref[i, 0], li_ref[i, 1], mh[:, lanes], ml[:, lanes])

    def values(v, t):
        parts = [
            back[128 * u + 8 * v : 128 * u + 8 * v + 8, columns(g, t)]
            for g in range(4)
            for u in range(2)
        ]
        return inverse8(*parts)

    over_x(0, slice(0, 128 * KERN))
    over_x(1, slice(columns(1, 0).start, columns(3, 1).stop))
    for v in range(16):
        for ch, (a, b) in enumerate(zip(values(v, 0), values(v, 1))):
            total[v, 8 * ch : 8 * ch + 8, :] = a * b
    over_x(1, slice(columns(1, 2).start, columns(3, 3).stop))
    for v in range(16):
        for ch, (a, b) in enumerate(zip(values(v, 2), values(v, 3))):
            total[v, 8 * ch : 8 * ch + 8, :] = total[v, 8 * ch : 8 * ch + 8, :] + a * b
    over_x(1, slice(columns(1, 4).start, columns(3, 4).stop))
    mask = mask_ref[...]
    for v in range(16):
        for ch, loss in enumerate(values(v, 4)):
            rows = slice(8 * ch, 8 * ch + 8)
            f = x_ref[THERE_AT[v], rows, :]
            out_ref[BACK_AT[v], rows, :] = f + mask * (total[v, rows, :] - f * loss)


def place_kernel(in_ref, out_ref, out, sem):
    stores = [
        pltpu.make_async_copy(out.at[pl.ds(8 * i, 8)], out_ref.at[pl.ds(8 * i, 8)], sem.at[i])
        for i in range(8)
    ]
    for tile in range(8):
        for x2 in range(2):
            for ch in range(8):
                j = 8 * x2 + ch
                for k in range(2):
                    at = BACK_AT[2 * tile + k] * SLOT + 8 * ch + x2
                    out[8 * tile + 4 * k : 8 * tile + 4 * k + 4, 128 * j : 128 * j + 128] = in_ref[
                        pl.ds(at, 4, stride=2), :
                    ]
        stores[tile].start()
    for copy in stores:
        copy.wait()


VM = pl.BlockSpec(memory_space=pltpu.VMEM)
SM = pl.BlockSpec(memory_space=pltpu.SMEM)
ANY = pl.BlockSpec(memory_space=pl.ANY)


def shape(*dims, dtype=F32):
    return jax.ShapeDtypeStruct(dims, dtype)


def params(mib):
    return pltpu.CompilerParams(vmem_limit_bytes=mib << 20)


def transport(side, courant, dist):
    return pl.pallas_call(
        transport_kernel,
        out_shape=[shape(16, SLOT, 128), shape(SLOT, 128)],
        in_specs=[SM, SM, VM],
        out_specs=[ANY, VM],
        scratch_shapes=[
            pltpu.VMEM((68 * 16, 128), F32),
            pltpu.VMEM((16, SLOT, 128), F32),
            pltpu.SemaphoreType.DMA((16,)),
        ],
        compiler_params=params(8),
        cost_estimate=pl.CostEstimate(flops=4000000, bytes_accessed=1 << 20, transcendentals=0),
        name="transport",
    )(side, courant, dist)


def edges(side, courant, edge, halo, mine):
    return pl.pallas_call(
        edge_kernel,
        out_shape=shape(16, SLOT, 128),
        in_specs=[SM, SM, VM, VM, ANY],
        out_specs=ANY,
        input_output_aliases={4: 0},
        scratch_shapes=[
            pltpu.VMEM((128, 128), F32),
            pltpu.VMEM((SLOT, 128), F32),
            pltpu.SemaphoreType.DMA,
        ],
        compiler_params=params(8),
        name="edges",
    )(side, courant, edge, halo, mine)


def make_tables(where, order, kernels):
    rows = pltpu.VMEM((KERN * 256, 128), F32)
    return pl.pallas_call(
        tables_kernel,
        out_shape=[shape(576, 128), shape(8, KERN, 32, 128), shape(8, 128)],
        in_specs=[SM] + [VM] * 3,
        out_specs=[VM] * 3,
        scratch_shapes=[rows, rows],
        compiler_params=params(12),
        cost_estimate=pl.CostEstimate(flops=8000000, bytes_accessed=4 << 20, transcendentals=0),
        name="tables",
    )(where, order, kernels, jnp.asarray(constant_rows()))


def collide(x, tables):
    left = pltpu.VMEM((2, 2, 256, 256), BF16)
    half = pltpu.VMEM((256, 512), BF16)
    field = pltpu.VMEM((512, 256), BF16)
    wide = pltpu.VMEM((256, 2560), BF16)
    return pl.pallas_call(
        collide_kernel,
        out_shape=shape(16, SLOT, 128),
        in_specs=[VM] * 4,
        out_specs=VM,
        scratch_shapes=[
            left,
            left,
            half,
            half,
            pltpu.VMEM((256, 512), F32),
            field,
            field,
            pltpu.VMEM((512, 256), F32),
            wide,
            wide,
            pltpu.VMEM((256, 2560), F32),
            pltpu.VMEM((16, SLOT, 128), F32),
        ],
        compiler_params=params(20),
        name="collide",
    )(x, *tables)


def place(x):
    return pl.pallas_call(
        place_kernel,
        out_shape=shape(64, 2048),
        in_specs=[VM],
        out_specs=ANY,
        scratch_shapes=[pltpu.VMEM((64, 2048), F32), pltpu.SemaphoreType.DMA((8,))],
        compiler_params=params(8),
        name="place",
    )(x.reshape(16 * SLOT, 128))


def exchange(slots, order):
    return lax.all_to_all(
        slots, "vel", split_axis=0, concat_axis=0, tiled=True, axis_index_groups=[list(order)]
    )


def local(distribution, collision_order, collision_blocks, kernels):
    v = lax.axis_index("vel")
    rising = v >= 8
    x = 2 * v + lax.iota(jnp.int32, 2)
    courant = jnp.abs(COURANT_MAX * (2.0 * x.astype(F32) - (NV - 1)) / (NV - 1))
    side = jnp.where(rising, -1, 1).astype(jnp.int32)[None]
    pairs = []
    for s in range(16):
        for u in range(16):
            to = s + 1 if u >= 8 else s - 1
            if 0 <= to < 16:
                pairs.append((s * 16 + u, to * 16 + u))
    send = jnp.where(rising, distribution[62:64], distribution[0:2])
    mine, edge = transport(side, courant, distribution)
    halo = lax.ppermute(send, ("space", "vel"), pairs)
    mine = edges(side, courant, edge, halo, mine)
    where = jnp.stack([v.astype(jnp.int32), collision_blocks[0]])
    tables = make_tables(where, collision_order, kernels)
    cells = exchange(mine, THERE)
    return place(exchange(collide(cells, tables), BACK))


def solution(mesh):
    in_specs = (P("space", "vel"), P("space", None), P("space"), P())
    out_specs = P("space", "vel")
    return jax.shard_map(local, mesh=mesh, in_specs=in_specs, out_specs=out_specs, check_vma=False)
```

```python
import math

import jax
import jax.numpy as jnp
import numpy as np
from jax import lax
from jax.experimental import pallas as pl
from jax.experimental.pallas import tpu as pltpu
from jax.sharding import PartitionSpec as P

NV = 32
BLOCK_CELLS = 16
KERN = 5
COURANT_MAX = 0.95
STEP_SCALE = 0.25
F32 = jnp.float32
BF16 = jnp.bfloat16
SLOT = 64

THERE = (10, 11, 14, 15, 9, 13, 6, 7, 0, 8, 12, 2, 3, 1, 4, 5)
BACK = (10, 15, 5, 0, 11, 14, 4, 1, 9, 12, 6, 3, 8, 13, 7, 2)
THERE_AT = [THERE.index(v) for v in range(16)]
BACK_AT = [BACK.index(v) for v in range(16)]


def constant_rows():
    lane = np.arange(128)
    y4, z = lane // 32, lane % 32
    x = 2 * (lane // 8) + lane % 2
    unit = 2.0 * math.pi / 32
    parts = []
    for phase in (8 * np.outer(y4, y4) + np.outer(z, z), np.outer(np.arange(32), x), np.outer(x, z)):
        parts += [np.cos((phase % 32) * unit), np.sin((phase % 32) * unit)]
    neg = (32 - z) % 32
    for other in ((4 - y4) % 4, 3 - y4):
        flip = np.zeros((128, 128))
        flip[other * 32 + neg, lane] = 1.0
        parts.append(flip)
    return np.concatenate(parts, axis=0).astype(np.float32)


def split(a):
    hi = a.astype(BF16)
    lo = (a - hi.astype(F32)).astype(BF16)
    return hi, lo


def dot(a, b):
    return jnp.dot(a, b, preferred_element_type=F32)


def dot3(ahi, alo, bhi, blo):
    return dot(ahi, bhi) + dot(ahi, blo) + dot(alo, bhi)


def upwind(near, info_ref, half):
    l2, l1, f0, r1, r2 = near
    rising = info_ref[0:8, :] > 0.0
    a = info_ref[8 + 8 * half : 16 + 8 * half, :]
    f1 = jnp.where(rising, l1, r1)
    f2 = jnp.where(rising, l2, r2)
    once = f0 - a * (f0 - f1)
    beside = f1 - a * (f1 - f2)
    return once - a * (once - beside)


def transport_kernel(info_ref, dist_ref, out_ref, edge_ref, raw, slots, out_sem):
    zero = jnp.zeros((32, 128), F32)
    raw[0:32, :] = zero
    raw[66 * 16 : 68 * 16, :] = zero
    for tile in range(8):
        for j in range(16):
            raw[pl.ds((8 * tile + 2) * 16 + j, 8, stride=16), :] = dist_ref[
                8 * tile : 8 * tile + 8, 128 * j : 128 * j + 128
            ]
    stores = [
        pltpu.make_async_copy(slots.at[i], out_ref.at[i], out_sem.at[i]) for i in range(16)
    ]
    for cell in range(64):
        for half in range(2):
            near = [raw[16 * (cell + k) + 8 * half : 16 * (cell + k) + 8 * half + 8, :] for k in range(5)]
            slots[THERE_AT[cell // 4], pl.ds(2 * (cell % 4) + half, 8, stride=8), :] = upwind(
                near, info_ref, half
            )
        if cell % 4 == 3:
            stores[THERE_AT[cell // 4]].start()
    edge_ref[0:96, :] = raw[32:128, :]
    edge_ref[96:192, :] = raw[60 * 16 : 66 * 16, :]
    for copy in stores:
        copy.wait()


def edge_kernel(info_ref, edge_ref, halo_ref, _, out_ref, left, right, slots, sem):
    left[32:128, :] = edge_ref[0:96, :]
    right[0:96, :] = edge_ref[96:192, :]
    for j in range(16):
        rows = halo_ref[:, 128 * j : 128 * j + 128]
        left[pl.ds(j, 2, stride=16), :] = rows
        right[pl.ds(96 + j, 2, stride=16), :] = rows
    copies = []
    for i, (raw, at) in enumerate(((left, THERE_AT[0]), (right, THERE_AT[15]))):
        for cell in range(4):
            for half in range(2):
                near = [
                    raw[16 * (cell + k) + 8 * half : 16 * (cell + k) + 8 * half + 8, :] for k in range(5)
                ]
                slots[i, pl.ds(2 * cell + half, 8, stride=8), :] = upwind(near, info_ref, half)
        copies.append(pltpu.make_async_copy(slots.at[i], out_ref.at[at], sem.at[i]))
        copies[-1].start()
    for copy in copies:
        copy.wait()


def tables_kernel(
    where_ref, order_ref, kern_ref, const_ref, base_ref, ks_ref, mask_ref, rows, turned
):
    position = lax.broadcasted_iota(jnp.int32, (1, 64), 1)
    first = position < BLOCK_CELLS * where_ref[1]
    for c in range(4):
        hit = jnp.where(first & (order_ref[...] == 4 * where_ref[0] + c), STEP_SCALE, 0.0)
        mask_ref[2 * c : 2 * c + 2, :] = jnp.broadcast_to(jnp.sum(hit, axis=1, keepdims=True), (2, 128))
    base_ref[...] = const_ref[0:576, :]
    for kx in range(32):
        for ch in range(8):
            at = kx * 8 + ch
            back = ((32 - kx) % 32) * 8 + ch
            tile = kern_ref[:, at * 128 : at * 128 + 128]
            rows[pl.ds(at, KERN, stride=256), :] = tile
            turned[pl.ds(back, KERN, stride=256), :] = tile
    group = lax.broadcasted_iota(jnp.int32, (32, 128), 1) // 32

    def ordered(src, t, k8):
        g, h = k8 % 4, k8 // 4
        out = None
        for k4 in range(4):
            piece = src[pl.ds(t * 256 + 2 * k4 + h, 32, stride=8), :]
            if k4 != g:
                piece = pltpu.roll(piece, ((k4 - g) % 4) * 32, 1)
            out = piece if out is None else jnp.where(group == k4, piece, out)
        return out

    scale = 0.5 / NV**3
    for k8 in range(8):
        at = 576 if k8 == 0 else 704
        flip = const_ref[at : at + 128, :].astype(BF16)
        for t in range(KERN):
            straight = ordered(rows, t, k8)
            other = ordered(turned, t, (8 - k8) % 8)
            hi, lo = split(other)
            ks_ref[k8, t] = scale * (straight + (dot(hi, flip) + dot(lo, flip)))


def turn(k8, lane_y4):
    cvec = jnp.full((1, 128), 1.0, F32)
    svec = jnp.full((1, 128), 0.0, F32)
    for y4 in range(1, 4):
        angle = 2 * math.pi * y4 * k8 / 32
        cvec = jnp.where(lane_y4 == y4, math.cos(angle), cvec)
        svec = jnp.where(lane_y4 == y4, math.sin(angle), svec)
    return cvec, svec


ROOT = math.sqrt(0.5)
PAIRS = ((0, 4), (1, 7), (2, 6), (3, 5))


def forward8(x):
    a = [x[j] + x[j + 4] for j in range(4)]
    d = [x[j] - x[j + 4] for j in range(4)]
    even, odd = a[0] + a[2], a[1] + a[3]
    less, more = ROOT * (d[1] - d[3]), ROOT * (d[1] + d[3])
    return (
        (even + odd, even - odd),
        (d[0] + less, -d[2] - more),
        (a[0] - a[2], a[3] - a[1]),
        (d[0] - less, d[2] - more),
    )


def inverse8(r0, r4, c1, s1, c2, s2, c3, s3):
    e, o = r0 + r4, r0 - r4
    a, b, c, d = e + c2, e - c2, c1 + c3, s3 - s1
    p, q = o - s2, o + s2
    less, more = ROOT * (c1 - c3), ROOT * (s1 + s3)
    m, n = less - more, less + more
    return [a + c, p + m, b + d, q - n, a - c, p - m, b - d, q + n]


def right(base_ref, k8, inverse):
    c, s = base_ref[0:128, :], base_ref[128:256, :]
    if k8:
        cvec, svec = turn(k8, lax.broadcasted_iota(jnp.int32, (1, 128), 1) // 32)
        c, s = cvec * c - svec * s, cvec * s + svec * c
    halves = []
    for c, s in zip(split(c), split(s)):
        up, down = (s, -s) if inverse else (-s, s)
        halves.append(
            jnp.concatenate(
                [jnp.concatenate([c, up], axis=1), jnp.concatenate([down, c], axis=1)], axis=0
            )
        )
    return halves


def left_matrices(base_ref, lf_ref, li_ref):
    zero = jnp.zeros((32, 128), BF16)
    c, s = base_ref[256:288, :], base_ref[288:320, :]
    cell = (lax.broadcasted_iota(jnp.int32, (32, 128), 1) % 8) // 2
    for p in range(2):
        first, second = cell == 2 * p, cell == 2 * p + 1
        real = split(jnp.where(first, c, jnp.where(second, s, 0.0)))
        imag = split(jnp.where(first, -s, jnp.where(second, c, 0.0)))
        for half in range(2):
            re, im = real[half], imag[half]
            for kk in range(2):
                at = 128 * kk + 64 * p
                top, low = slice(at, at + 32), slice(at + 32, at + 64)
                mine, other = slice(128 * kk, 128 * kk + 128), slice(128 - 128 * kk, 256 - 128 * kk)
                lf_ref[0, half, top, mine], lf_ref[0, half, low, mine] = re, im
                lf_ref[0, half, top, other], lf_ref[0, half, low, other] = zero, zero
                lf_ref[1, half, top, 0:128], lf_ref[1, half, low, 0:128] = re, im
                lf_ref[1, half, top, 128:256] = im if kk else -im
                lf_ref[1, half, low, 128:256] = -re if kk else re
    zero = jnp.zeros((128, 128), BF16)
    c, s = base_ref[320:448, :], base_ref[448:576, :]
    cell = (lax.broadcasted_iota(jnp.int32, (128, 128), 0) % 8) // 2
    lane = lax.broadcasted_iota(jnp.int32, (128, 128), 1)
    first, second = cell == 2 * (lane // 64), cell == 2 * (lane // 64) + 1
    real = (lane // 32) % 2 == 0
    zeroth = split(jnp.where(first, jnp.where(real, c, -s), jnp.where(second, jnp.where(real, s, c), 0.0)))
    other = split(jnp.where(first, jnp.where(real, s, c), jnp.where(second, jnp.where(real, -c, s), 0.0)))
    for half in range(2):
        a, b = zeroth[half], other[half]
        up, low = slice(0, 128), slice(128, 256)
        li_ref[0, half, up, up], li_ref[0, half, up, low] = a, zero
        li_ref[0, half, low, up], li_ref[0, half, low, low] = zero, a
        li_ref[1, half, up, up], li_ref[1, half, up, low] = a, a
        li_ref[1, half, low, up], li_ref[1, half, low, low] = b, -b


def columns(g, t):
    at = 128 * (t if g == 0 else KERN + 3 * t + g - 1)
    return slice(at, at + 128)


def collide_kernel(
    x_ref, base_ref, ks_ref, mask_ref, out_ref, lf_ref, li_ref, fh, fl, y, gh, gl, spec, mh, ml, back, total
):
    left_matrices(base_ref, lf_ref, li_ref)
    for v in range(0, 16, 2):
        x = [
            jnp.concatenate(
                [x_ref[THERE_AT[v + i], 8 * ch : 8 * ch + 8, :] for i in range(2)], axis=0
            )
            for ch in range(8)
        ]
        for g, parts in enumerate(forward8(x)):
            for u, part in enumerate(parts):
                rows, lanes = slice(128 * u + 8 * v, 128 * u + 8 * v + 16), slice(128 * g, 128 * g + 128)
                fh[rows, lanes], fl[rows, lanes] = split(part)
    for i, lanes in enumerate((slice(0, 128), slice(128, 512))):
        y[:, lanes] = dot3(lf_ref[i, 0], lf_ref[i, 1], fh[:, lanes], fl[:, lanes])
    lane_y4 = lax.broadcasted_iota(jnp.int32, (1, 128), 1) // 32
    for g in range(4):
        for kk in range(2):
            k8 = PAIRS[g][kk]
            cvec, svec = turn(k8, lane_y4)
            for p in range(2):
                at = 128 * kk + 64 * p
                lanes = slice(128 * g, 128 * g + 128)
                re, im = y[at : at + 32, lanes], y[at + 32 : at + 64, lanes]
                if k8:
                    re, im = re * cvec + im * svec, im * cvec - re * svec
                rows = slice(64 * k8 + 32 * p, 64 * k8 + 32 * p + 32)
                gh[rows, 0:128], gl[rows, 0:128] = split(re)
                gh[rows, 128:256], gl[rows, 128:256] = split(im)
    spec[...] = dot3(gh[...], gl[...], *right(base_ref, 0, False))
    for g in range(4):
        for kk in range(2):
            k8 = PAIRS[g][kk]
            parts = []
            for t in range(KERN):
                ks = ks_ref[k8, t]
                ks = jnp.concatenate([ks, ks], axis=1)
                for p in range(2):
                    at = 64 * k8 + 32 * p
                    parts.append(spec[at : at + 32, :] * ks)
            hi, lo = split(jnp.concatenate(parts, axis=0))
            done = dot3(hi, lo, *right(base_ref, k8, True))
            hi, lo = split(done)
            for n in range(2 * KERN):
                t, p = n // 2, n % 2
                for ri in range(2):
                    at = 128 * kk + 64 * p + 32 * ri
                    part = (slice(32 * n, 32 * n + 32), slice(128 * ri, 128 * ri + 128))
                    mh[at : at + 32, columns(g, t)] = hi[part]
                    ml[at : at + 32, columns(g, t)] = lo[part]

    def over_x(i, lanes):
        back[:, lanes] = dot3(li_ref[i, 0], li_ref[i, 1], mh[:, lanes], ml[:, lanes])

    def values(v, t):
        parts = [
            back[128 * u + 8 * v : 128 * u + 8 * v + 8, columns(g, t)]
            for g in range(4)
            for u in range(2)
        ]
        return inverse8(*parts)

    over_x(0, slice(0, 128 * KERN))
    over_x(1, slice(columns(1, 0).start, columns(3, 1).stop))
    for v in range(16):
        for ch, (a, b) in enumerate(zip(values(v, 0), values(v, 1))):
            total[v, 8 * ch : 8 * ch + 8, :] = a * b
    over_x(1, slice(columns(1, 2).start, columns(3, 3).stop))
    for v in range(16):
        for ch, (a, b) in enumerate(zip(values(v, 2), values(v, 3))):
            total[v, 8 * ch : 8 * ch + 8, :] = total[v, 8 * ch : 8 * ch + 8, :] + a * b
    over_x(1, slice(columns(1, 4).start, columns(3, 4).stop))
    mask = mask_ref[...]
    for v in range(16):
        for ch, loss in enumerate(values(v, 4)):
            rows = slice(8 * ch, 8 * ch + 8)
            f = x_ref[THERE_AT[v], rows, :]
            out_ref[BACK_AT[v], rows, :] = f + mask * (total[v, rows, :] - f * loss)


def place_kernel(in_ref, out_ref, out, sem):
    stores = [
        pltpu.make_async_copy(out.at[pl.ds(8 * i, 8)], out_ref.at[pl.ds(8 * i, 8)], sem.at[i])
        for i in range(8)
    ]
    for tile in range(8):
        for x2 in range(2):
            for ch in range(8):
                j = 8 * x2 + ch
                for k in range(2):
                    at = BACK_AT[2 * tile + k] * SLOT + 8 * ch + x2
                    out[8 * tile + 4 * k : 8 * tile + 4 * k + 4, 128 * j : 128 * j + 128] = in_ref[
                        pl.ds(at, 4, stride=2), :
                    ]
        stores[tile].start()
    for copy in stores:
        copy.wait()


VM = pl.BlockSpec(memory_space=pltpu.VMEM)
SM = pl.BlockSpec(memory_space=pltpu.SMEM)
ANY = pl.BlockSpec(memory_space=pl.ANY)


def shape(*dims, dtype=F32):
    return jax.ShapeDtypeStruct(dims, dtype)


def params(mib):
    return pltpu.CompilerParams(vmem_limit_bytes=mib << 20)


def transport(info, dist):
    return pl.pallas_call(
        transport_kernel,
        out_shape=[shape(16, SLOT, 128), shape(192, 128)],
        in_specs=[VM, VM],
        out_specs=[ANY, VM],
        scratch_shapes=[
            pltpu.VMEM((68 * 16, 128), F32),
            pltpu.VMEM((16, SLOT, 128), F32),
            pltpu.SemaphoreType.DMA((16,)),
        ],
        compiler_params=params(8),
        cost_estimate=pl.CostEstimate(flops=4000000, bytes_accessed=1 << 20, transcendentals=0),
        name="transport",
    )(info, dist)


def edges(info, edge, halo, mine):
    return pl.pallas_call(
        edge_kernel,
        out_shape=shape(16, SLOT, 128),
        in_specs=[VM, VM, VM, ANY],
        out_specs=ANY,
        input_output_aliases={3: 0},
        scratch_shapes=[
            pltpu.VMEM((128, 128), F32),
            pltpu.VMEM((128, 128), F32),
            pltpu.VMEM((2, SLOT, 128), F32),
            pltpu.SemaphoreType.DMA((2,)),
        ],
        compiler_params=params(8),
        name="edges",
    )(info, edge, halo, mine)


def make_tables(where, order, kernels):
    rows = pltpu.VMEM((KERN * 256, 128), F32)
    return pl.pallas_call(
        tables_kernel,
        out_shape=[shape(576, 128), shape(8, KERN, 32, 128), shape(8, 128)],
        in_specs=[SM] + [VM] * 3,
        out_specs=[VM] * 3,
        scratch_shapes=[rows, rows],
        compiler_params=params(12),
        cost_estimate=pl.CostEstimate(flops=8000000, bytes_accessed=4 << 20, transcendentals=0),
        name="tables",
    )(where, order, kernels, jnp.asarray(constant_rows()))


def collide(x, tables):
    left = pltpu.VMEM((2, 2, 256, 256), BF16)
    half = pltpu.VMEM((256, 512), BF16)
    field = pltpu.VMEM((512, 256), BF16)
    wide = pltpu.VMEM((256, 2560), BF16)
    return pl.pallas_call(
        collide_kernel,
        out_shape=shape(16, SLOT, 128),
        in_specs=[VM] * 4,
        out_specs=VM,
        scratch_shapes=[
            left,
            left,
            half,
            half,
            pltpu.VMEM((256, 512), F32),
            field,
            field,
            pltpu.VMEM((512, 256), F32),
            wide,
            wide,
            pltpu.VMEM((256, 2560), F32),
            pltpu.VMEM((16, SLOT, 128), F32),
        ],
        compiler_params=params(20),
        name="collide",
    )(x, *tables)


def place(x):
    return pl.pallas_call(
        place_kernel,
        out_shape=shape(64, 2048),
        in_specs=[VM],
        out_specs=ANY,
        scratch_shapes=[pltpu.VMEM((64, 2048), F32), pltpu.SemaphoreType.DMA((8,))],
        compiler_params=params(8),
        name="place",
    )(x.reshape(16 * SLOT, 128))


def exchange(slots, order):
    return lax.all_to_all(
        slots, "vel", split_axis=0, concat_axis=0, tiled=True, axis_index_groups=[list(order)]
    )


def local(distribution, collision_order, collision_blocks, kernels):
    v = lax.axis_index("vel")
    rising = v >= 8
    row = lax.broadcasted_iota(jnp.int32, (24, 128), 0)
    x = (2 * v + (row >= 16)).astype(F32)
    courant = jnp.abs(COURANT_MAX * (2.0 * x - (NV - 1)) / (NV - 1))
    info = jnp.where(row < 8, jnp.where(rising, 1.0, -1.0), courant)
    pairs = []
    for s in range(16):
        for u in range(16):
            to = s + 1 if u >= 8 else s - 1
            if 0 <= to < 16:
                pairs.append((s * 16 + u, to * 16 + u))
    send = jnp.where(rising, distribution[62:64], distribution[0:2])
    mine, edge = transport(info, distribution)
    halo = lax.ppermute(send, ("space", "vel"), pairs)
    mine = edges(info, edge, halo, mine)
    where = jnp.stack([v.astype(jnp.int32), collision_blocks[0]])
    tables = make_tables(where, collision_order, kernels)
    cells = exchange(mine, THERE)
    return place(exchange(collide(cells, tables), BACK))


def solution(mesh):
    in_specs = (P("space", "vel"), P("space", None), P("space"), P())
    out_specs = P("space", "vel")
    return jax.shard_map(local, mesh=mesh, in_specs=in_specs, out_specs=out_specs, check_vma=False)
```

```python
import math

import jax
import jax.numpy as jnp
import numpy as np
from jax import lax
from jax.experimental import pallas as pl
from jax.experimental.pallas import tpu as pltpu
from jax.sharding import PartitionSpec as P

NV = 32
BLOCK_CELLS = 16
KERN = 5
COURANT_MAX = 0.95
STEP_SCALE = 0.25
F32 = jnp.float32
BF16 = jnp.bfloat16
SLOT = 64

THERE = (10, 11, 2, 15, 9, 13, 6, 7, 0, 8, 12, 14, 3, 1, 4, 5)
BACK = (10, 15, 5, 3, 11, 14, 4, 1, 9, 12, 6, 2, 8, 13, 7, 0)
THERE_AT = [THERE.index(v) for v in range(16)]
BACK_AT = [BACK.index(v) for v in range(16)]


def constant_rows():
    lane = np.arange(128)
    y4, z = lane // 32, lane % 32
    x = 2 * (lane // 8) + lane % 2
    unit = 2.0 * math.pi / 32
    parts = []
    for phase in (8 * np.outer(y4, y4) + np.outer(z, z), np.outer(np.arange(32), x), np.outer(x, z)):
        parts += [np.cos((phase % 32) * unit), np.sin((phase % 32) * unit)]
    neg = (32 - z) % 32
    for other in ((4 - y4) % 4, 3 - y4):
        flip = np.zeros((128, 128))
        flip[other * 32 + neg, lane] = 1.0
        parts.append(flip)
    return np.concatenate(parts, axis=0).astype(np.float32)


def split(a):
    hi = a.astype(BF16)
    lo = (a - hi.astype(F32)).astype(BF16)
    return hi, lo


def dot(a, b):
    return jnp.dot(a, b, preferred_element_type=F32)


def dot3(ahi, alo, bhi, blo):
    return dot(ahi, bhi) + dot(ahi, blo) + dot(alo, bhi)


def upwind(near, info_ref, half):
    l2, l1, f0, r1, r2 = near
    rising = info_ref[0:8, :] > 0.0
    a = info_ref[8 + 8 * half : 16 + 8 * half, :]
    f1 = jnp.where(rising, l1, r1)
    f2 = jnp.where(rising, l2, r2)
    once = f0 - a * (f0 - f1)
    beside = f1 - a * (f1 - f2)
    return once - a * (once - beside)


def transport_kernel(info_ref, dist_ref, out_ref, edge_ref, raw, slots, out_sem):
    zero = jnp.zeros((32, 128), F32)
    raw[0:32, :] = zero
    raw[66 * 16 : 68 * 16, :] = zero
    for tile in range(8):
        for j in range(16):
            raw[pl.ds((8 * tile + 2) * 16 + j, 8, stride=16), :] = dist_ref[
                8 * tile : 8 * tile + 8, 128 * j : 128 * j + 128
            ]
    stores = [
        pltpu.make_async_copy(slots.at[i], out_ref.at[i], out_sem.at[i]) for i in range(16)
    ]
    for cell in range(64):
        for half in range(2):
            near = [raw[16 * (cell + k) + 8 * half : 16 * (cell + k) + 8 * half + 8, :] for k in range(5)]
            slots[THERE_AT[cell // 4], pl.ds(2 * (cell % 4) + half, 8, stride=8), :] = upwind(
                near, info_ref, half
            )
        if cell % 4 == 3:
            stores[THERE_AT[cell // 4]].start()
    edge_ref[0:96, :] = raw[32:128, :]
    edge_ref[96:192, :] = raw[60 * 16 : 66 * 16, :]
    for copy in stores:
        copy.wait()


def edge_kernel(info_ref, edge_ref, halo_ref, _, out_ref, left, right, slots, sem):
    left[32:128, :] = edge_ref[0:96, :]
    right[0:96, :] = edge_ref[96:192, :]
    for j in range(16):
        rows = halo_ref[:, 128 * j : 128 * j + 128]
        left[pl.ds(j, 2, stride=16), :] = rows
        right[pl.ds(96 + j, 2, stride=16), :] = rows
    copies = []
    for i, (raw, at) in enumerate(((left, THERE_AT[0]), (right, THERE_AT[15]))):
        for cell in range(4):
            for half in range(2):
                near = [
                    raw[16 * (cell + k) + 8 * half : 16 * (cell + k) + 8 * half + 8, :] for k in range(5)
                ]
                slots[i, pl.ds(2 * cell + half, 8, stride=8), :] = upwind(near, info_ref, half)
        copies.append(pltpu.make_async_copy(slots.at[i], out_ref.at[at], sem.at[i]))
        copies[-1].start()
    for copy in copies:
        copy.wait()


def tables_kernel(
    where_ref, order_ref, kern_ref, const_ref, base_ref, ks_ref, mask_ref, rows, turned
):
    position = lax.broadcasted_iota(jnp.int32, (1, 64), 1)
    first = position < BLOCK_CELLS * where_ref[1]
    for c in range(4):
        hit = jnp.where(first & (order_ref[...] == 4 * where_ref[0] + c), STEP_SCALE, 0.0)
        mask_ref[2 * c : 2 * c + 2, :] = jnp.broadcast_to(jnp.sum(hit, axis=1, keepdims=True), (2, 128))
    base_ref[...] = const_ref[0:576, :]
    for kx in range(32):
        for ch in range(8):
            at = kx * 8 + ch
            back = ((32 - kx) % 32) * 8 + ch
            tile = kern_ref[:, at * 128 : at * 128 + 128]
            rows[pl.ds(at, KERN, stride=256), :] = tile
            turned[pl.ds(back, KERN, stride=256), :] = tile
    group = lax.broadcasted_iota(jnp.int32, (32, 128), 1) // 32

    def ordered(src, t, k8):
        g, h = k8 % 4, k8 // 4
        out = None
        for k4 in range(4):
            piece = src[pl.ds(t * 256 + 2 * k4 + h, 32, stride=8), :]
            if k4 != g:
                piece = pltpu.roll(piece, ((k4 - g) % 4) * 32, 1)
            out = piece if out is None else jnp.where(group == k4, piece, out)
        return out

    scale = 0.5 / NV**3
    for k8 in range(8):
        at = 576 if k8 == 0 else 704
        flip = const_ref[at : at + 128, :].astype(BF16)
        for t in range(KERN):
            straight = ordered(rows, t, k8)
            other = ordered(turned, t, (8 - k8) % 8)
            hi, lo = split(other)
            ks_ref[k8, t] = scale * (straight + (dot(hi, flip) + dot(lo, flip)))


def turn(k8, lane_y4):
    cvec = jnp.full((1, 128), 1.0, F32)
    svec = jnp.full((1, 128), 0.0, F32)
    for y4 in range(1, 4):
        angle = 2 * math.pi * y4 * k8 / 32
        cvec = jnp.where(lane_y4 == y4, math.cos(angle), cvec)
        svec = jnp.where(lane_y4 == y4, math.sin(angle), svec)
    return cvec, svec


ROOT = math.sqrt(0.5)
PAIRS = ((0, 4), (1, 7), (2, 6), (3, 5))


def forward8(x):
    a = [x[j] + x[j + 4] for j in range(4)]
    d = [x[j] - x[j + 4] for j in range(4)]
    even, odd = a[0] + a[2], a[1] + a[3]
    less, more = ROOT * (d[1] - d[3]), ROOT * (d[1] + d[3])
    return (
        (even + odd, even - odd),
        (d[0] + less, -d[2] - more),
        (a[0] - a[2], a[3] - a[1]),
        (d[0] - less, d[2] - more),
    )


def inverse8(r0, r4, c1, s1, c2, s2, c3, s3):
    e, o = r0 + r4, r0 - r4
    a, b, c, d = e + c2, e - c2, c1 + c3, s3 - s1
    p, q = o - s2, o + s2
    less, more = ROOT * (c1 - c3), ROOT * (s1 + s3)
    m, n = less - more, less + more
    return [a + c, p + m, b + d, q - n, a - c, p - m, b - d, q + n]


def right(base_ref, k8, inverse):
    c, s = base_ref[0:128, :], base_ref[128:256, :]
    if k8:
        cvec, svec = turn(k8, lax.broadcasted_iota(jnp.int32, (1, 128), 1) // 32)
        c, s = cvec * c - svec * s, cvec * s + svec * c
    halves = []
    for c, s in zip(split(c), split(s)):
        up, down = (s, -s) if inverse else (-s, s)
        halves.append(
            jnp.concatenate(
                [jnp.concatenate([c, up], axis=1), jnp.concatenate([down, c], axis=1)], axis=0
            )
        )
    return halves


def left_matrices(base_ref, lf_ref, li_ref):
    zero = jnp.zeros((32, 128), BF16)
    c, s = base_ref[256:288, :], base_ref[288:320, :]
    cell = (lax.broadcasted_iota(jnp.int32, (32, 128), 1) % 8) // 2
    for p in range(2):
        first, second = cell == 2 * p, cell == 2 * p + 1
        real = split(jnp.where(first, c, jnp.where(second, s, 0.0)))
        imag = split(jnp.where(first, -s, jnp.where(second, c, 0.0)))
        for half in range(2):
            re, im = real[half], imag[half]
            for kk in range(2):
                at = 128 * kk + 64 * p
                top, low = slice(at, at + 32), slice(at + 32, at + 64)
                mine, other = slice(128 * kk, 128 * kk + 128), slice(128 - 128 * kk, 256 - 128 * kk)
                lf_ref[0, half, top, mine], lf_ref[0, half, low, mine] = re, im
                lf_ref[0, half, top, other], lf_ref[0, half, low, other] = zero, zero
                lf_ref[1, half, top, 0:128], lf_ref[1, half, low, 0:128] = re, im
                lf_ref[1, half, top, 128:256] = im if kk else -im
                lf_ref[1, half, low, 128:256] = -re if kk else re
    zero = jnp.zeros((128, 128), BF16)
    c, s = base_ref[320:448, :], base_ref[448:576, :]
    cell = (lax.broadcasted_iota(jnp.int32, (128, 128), 0) % 8) // 2
    lane = lax.broadcasted_iota(jnp.int32, (128, 128), 1)
    first, second = cell == 2 * (lane // 64), cell == 2 * (lane // 64) + 1
    real = (lane // 32) % 2 == 0
    zeroth = split(jnp.where(first, jnp.where(real, c, -s), jnp.where(second, jnp.where(real, s, c), 0.0)))
    other = split(jnp.where(first, jnp.where(real, s, c), jnp.where(second, jnp.where(real, -c, s), 0.0)))
    for half in range(2):
        a, b = zeroth[half], other[half]
        up, low = slice(0, 128), slice(128, 256)
        li_ref[0, half, up, up], li_ref[0, half, up, low] = a, zero
        li_ref[0, half, low, up], li_ref[0, half, low, low] = zero, a
        li_ref[1, half, up, up], li_ref[1, half, up, low] = a, a
        li_ref[1, half, low, up], li_ref[1, half, low, low] = b, -b


def columns(g, t):
    at = 128 * (t if g == 0 else KERN + 3 * t + g - 1)
    return slice(at, at + 128)


def collide_kernel(
    x_ref, base_ref, ks_ref, mask_ref, out_ref, lf_ref, li_ref, fh, fl, y, gh, gl, spec, mh, ml, back, total
):
    left_matrices(base_ref, lf_ref, li_ref)
    for v in range(0, 16, 2):
        x = [
            jnp.concatenate(
                [x_ref[THERE_AT[v + i], 8 * ch : 8 * ch + 8, :] for i in range(2)], axis=0
            )
            for ch in range(8)
        ]
        for g, parts in enumerate(forward8(x)):
            for u, part in enumerate(parts):
                rows, lanes = slice(128 * u + 8 * v, 128 * u + 8 * v + 16), slice(128 * g, 128 * g + 128)
                fh[rows, lanes], fl[rows, lanes] = split(part)
    for i, lanes in enumerate((slice(0, 128), slice(128, 512))):
        y[:, lanes] = dot3(lf_ref[i, 0], lf_ref[i, 1], fh[:, lanes], fl[:, lanes])
    lane_y4 = lax.broadcasted_iota(jnp.int32, (1, 128), 1) // 32
    for g in range(4):
        for kk in range(2):
            k8 = PAIRS[g][kk]
            cvec, svec = turn(k8, lane_y4)
            for p in range(2):
                at = 128 * kk + 64 * p
                lanes = slice(128 * g, 128 * g + 128)
                re, im = y[at : at + 32, lanes], y[at + 32 : at + 64, lanes]
                if k8:
                    re, im = re * cvec + im * svec, im * cvec - re * svec
                rows = slice(64 * k8 + 32 * p, 64 * k8 + 32 * p + 32)
                gh[rows, 0:128], gl[rows, 0:128] = split(re)
                gh[rows, 128:256], gl[rows, 128:256] = split(im)
    spec[...] = dot3(gh[...], gl[...], *right(base_ref, 0, False))
    for g in range(4):
        for kk in range(2):
            k8 = PAIRS[g][kk]
            parts = []
            for t in range(KERN):
                ks = ks_ref[k8, t]
                ks = jnp.concatenate([ks, ks], axis=1)
                for p in range(2):
                    at = 64 * k8 + 32 * p
                    parts.append(spec[at : at + 32, :] * ks)
            hi, lo = split(jnp.concatenate(parts, axis=0))
            done = dot3(hi, lo, *right(base_ref, k8, True))
            hi, lo = split(done)
            for n in range(2 * KERN):
                t, p = n // 2, n % 2
                for ri in range(2):
                    at = 128 * kk + 64 * p + 32 * ri
                    part = (slice(32 * n, 32 * n + 32), slice(128 * ri, 128 * ri + 128))
                    mh[at : at + 32, columns(g, t)] = hi[part]
                    ml[at : at + 32, columns(g, t)] = lo[part]

    def over_x(i, lanes):
        back[:, lanes] = dot3(li_ref[i, 0], li_ref[i, 1], mh[:, lanes], ml[:, lanes])

    def values(v, t):
        parts = [
            back[128 * u + 8 * v : 128 * u + 8 * v + 8, columns(g, t)]
            for g in range(4)
            for u in range(2)
        ]
        return inverse8(*parts)

    over_x(0, slice(0, 128 * KERN))
    over_x(1, slice(columns(1, 0).start, columns(3, 1).stop))
    for v in range(16):
        for ch, (a, b) in enumerate(zip(values(v, 0), values(v, 1))):
            total[v, 8 * ch : 8 * ch + 8, :] = a * b
    over_x(1, slice(columns(1, 2).start, columns(3, 3).stop))
    for v in range(16):
        for ch, (a, b) in enumerate(zip(values(v, 2), values(v, 3))):
            total[v, 8 * ch : 8 * ch + 8, :] = total[v, 8 * ch : 8 * ch + 8, :] + a * b
    over_x(1, slice(columns(1, 4).start, columns(3, 4).stop))
    mask = mask_ref[...]
    for v in range(16):
        for ch, loss in enumerate(values(v, 4)):
            rows = slice(8 * ch, 8 * ch + 8)
            f = x_ref[THERE_AT[v], rows, :]
            out_ref[BACK_AT[v], rows, :] = f + mask * (total[v, rows, :] - f * loss)


def place_kernel(in_ref, out_ref, out, sem):
    stores = [
        pltpu.make_async_copy(out.at[pl.ds(8 * i, 8)], out_ref.at[pl.ds(8 * i, 8)], sem.at[i])
        for i in range(8)
    ]
    for tile in range(8):
        for x2 in range(2):
            for ch in range(8):
                j = 8 * x2 + ch
                for k in range(2):
                    at = BACK_AT[2 * tile + k] * SLOT + 8 * ch + x2
                    out[8 * tile + 4 * k : 8 * tile + 4 * k + 4, 128 * j : 128 * j + 128] = in_ref[
                        pl.ds(at, 4, stride=2), :
                    ]
        stores[tile].start()
    for copy in stores:
        copy.wait()


VM = pl.BlockSpec(memory_space=pltpu.VMEM)
SM = pl.BlockSpec(memory_space=pltpu.SMEM)
ANY = pl.BlockSpec(memory_space=pl.ANY)


def shape(*dims, dtype=F32):
    return jax.ShapeDtypeStruct(dims, dtype)


def params(mib):
    return pltpu.CompilerParams(vmem_limit_bytes=mib << 20)


def transport(info, dist):
    return pl.pallas_call(
        transport_kernel,
        out_shape=[shape(16, SLOT, 128), shape(192, 128)],
        in_specs=[VM, VM],
        out_specs=[ANY, VM],
        scratch_shapes=[
            pltpu.VMEM((68 * 16, 128), F32),
            pltpu.VMEM((16, SLOT, 128), F32),
            pltpu.SemaphoreType.DMA((16,)),
        ],
        compiler_params=params(8),
        cost_estimate=pl.CostEstimate(flops=4000000, bytes_accessed=1 << 20, transcendentals=0),
        name="transport",
    )(info, dist)


def edges(info, edge, halo, mine):
    return pl.pallas_call(
        edge_kernel,
        out_shape=shape(16, SLOT, 128),
        in_specs=[VM, VM, VM, ANY],
        out_specs=ANY,
        input_output_aliases={3: 0},
        scratch_shapes=[
            pltpu.VMEM((128, 128), F32),
            pltpu.VMEM((128, 128), F32),
            pltpu.VMEM((2, SLOT, 128), F32),
            pltpu.SemaphoreType.DMA((2,)),
        ],
        compiler_params=params(8),
        name="edges",
    )(info, edge, halo, mine)


def make_tables(where, order, kernels):
    rows = pltpu.VMEM((KERN * 256, 128), F32)
    return pl.pallas_call(
        tables_kernel,
        out_shape=[shape(576, 128), shape(8, KERN, 32, 128), shape(8, 128)],
        in_specs=[SM] + [VM] * 3,
        out_specs=[VM] * 3,
        scratch_shapes=[rows, rows],
        compiler_params=params(12),
        cost_estimate=pl.CostEstimate(flops=8000000, bytes_accessed=4 << 20, transcendentals=0),
        name="tables",
    )(where, order, kernels, jnp.asarray(constant_rows()))


def collide(x, tables):
    left = pltpu.VMEM((2, 2, 256, 256), BF16)
    half = pltpu.VMEM((256, 512), BF16)
    field = pltpu.VMEM((512, 256), BF16)
    wide = pltpu.VMEM((256, 2560), BF16)
    return pl.pallas_call(
        collide_kernel,
        out_shape=shape(16, SLOT, 128),
        in_specs=[VM] * 4,
        out_specs=VM,
        scratch_shapes=[
            left,
            left,
            half,
            half,
            pltpu.VMEM((256, 512), F32),
            field,
            field,
            pltpu.VMEM((512, 256), F32),
            wide,
            wide,
            pltpu.VMEM((256, 2560), F32),
            pltpu.VMEM((16, SLOT, 128), F32),
        ],
        compiler_params=pltpu.CompilerParams(
            vmem_limit_bytes=20 << 20
        ),
        name="collide",
    )(x, *tables)


def place(x):
    return pl.pallas_call(
        place_kernel,
        out_shape=shape(64, 2048),
        in_specs=[VM],
        out_specs=ANY,
        scratch_shapes=[pltpu.VMEM((64, 2048), F32), pltpu.SemaphoreType.DMA((8,))],
        compiler_params=params(8),
        name="place",
    )(x.reshape(16 * SLOT, 128))


def exchange(slots, order):
    return lax.all_to_all(
        slots, "vel", split_axis=0, concat_axis=0, tiled=True, axis_index_groups=[list(order)]
    )


def local(distribution, collision_order, collision_blocks, kernels):
    v = lax.axis_index("vel")
    rising = v >= 8
    row = lax.broadcasted_iota(jnp.int32, (24, 128), 0)
    x = (2 * v + (row >= 16)).astype(F32)
    courant = jnp.abs(COURANT_MAX * (2.0 * x - (NV - 1)) / (NV - 1))
    info = jnp.where(row < 8, jnp.where(rising, 1.0, -1.0), courant)
    pairs = []
    for s in range(16):
        for u in range(16):
            to = s + 1 if u >= 8 else s - 1
            if 0 <= to < 16:
                pairs.append((s * 16 + u, to * 16 + u))
    send = jnp.where(rising, distribution[62:64], distribution[0:2])
    mine, edge = transport(info, distribution)
    halo = lax.ppermute(send, ("space", "vel"), pairs)
    mine = edges(info, edge, halo, mine)
    where = jnp.stack([v.astype(jnp.int32), collision_blocks[0]])
    tables = make_tables(where, collision_order, kernels)
    cells = exchange(mine, THERE)
    return place(exchange(collide(cells, tables), BACK))


def solution(mesh):
    in_specs = (P("space", "vel"), P("space", None), P("space"), P())
    out_specs = P("space", "vel")
    return jax.shard_map(local, mesh=mesh, in_specs=in_specs, out_specs=out_specs, check_vma=False)
```

```python
import math

import jax
import jax.numpy as jnp
import numpy as np
from jax import lax
from jax.experimental import pallas as pl
from jax.experimental.pallas import tpu as pltpu
from jax.sharding import PartitionSpec as P

NV = 32
BLOCK_CELLS = 16
KERN = 5
COURANT_MAX = 0.95
STEP_SCALE = 0.25
F32 = jnp.float32
BF16 = jnp.bfloat16
SLOT = 64

THERE = (10, 11, 2, 15, 9, 13, 6, 7, 0, 8, 12, 14, 3, 1, 4, 5)
BACK = (10, 15, 5, 3, 11, 14, 4, 1, 9, 12, 6, 2, 8, 13, 7, 0)
THERE_AT = [THERE.index(v) for v in range(16)]
BACK_AT = [BACK.index(v) for v in range(16)]


def constant_rows():
    lane = np.arange(128)
    y4, z = lane // 32, lane % 32
    x = 2 * (lane // 8) + lane % 2
    unit = 2.0 * math.pi / 32
    parts = []
    for phase in (8 * np.outer(y4, y4) + np.outer(z, z), np.outer(np.arange(32), x), np.outer(x, z)):
        parts += [np.cos((phase % 32) * unit), np.sin((phase % 32) * unit)]
    neg = (32 - z) % 32
    for other in ((4 - y4) % 4, 3 - y4):
        flip = np.zeros((128, 128))
        flip[other * 32 + neg, lane] = 1.0
        parts.append(flip)
    return np.concatenate(parts, axis=0).astype(np.float32)


def split(a):
    hi = a.astype(BF16)
    lo = (a - hi.astype(F32)).astype(BF16)
    return hi, lo


def dot(a, b):
    return jnp.dot(a, b, preferred_element_type=F32)


def dot3(ahi, alo, bhi, blo):
    return dot(ahi, bhi) + dot(ahi, blo) + dot(alo, bhi)


def upwind(near, info_ref, half):
    l2, l1, f0, r1, r2 = near
    rising = info_ref[0:8, :] > 0.0
    a = info_ref[8 + 8 * half : 16 + 8 * half, :]
    f1 = jnp.where(rising, l1, r1)
    f2 = jnp.where(rising, l2, r2)
    once = f0 - a * (f0 - f1)
    beside = f1 - a * (f1 - f2)
    return once - a * (once - beside)


def transport_kernel(info_ref, dist_ref, out_ref, edge_ref, raw, slots, out_sem):
    zero = jnp.zeros((32, 128), F32)
    raw[0:32, :] = zero
    raw[66 * 16 : 68 * 16, :] = zero
    for tile in range(8):
        for j in range(16):
            raw[pl.ds((8 * tile + 2) * 16 + j, 8, stride=16), :] = dist_ref[
                8 * tile : 8 * tile + 8, 128 * j : 128 * j + 128
            ]
    stores = [
        pltpu.make_async_copy(slots.at[i], out_ref.at[i], out_sem.at[i]) for i in range(16)
    ]
    for cell in range(64):
        for half in range(2):
            near = [raw[16 * (cell + k) + 8 * half : 16 * (cell + k) + 8 * half + 8, :] for k in range(5)]
            slots[THERE_AT[cell // 4], pl.ds(2 * (cell % 4) + half, 8, stride=8), :] = upwind(
                near, info_ref, half
            )
        if cell % 4 == 3:
            stores[THERE_AT[cell // 4]].start()
    edge_ref[0:96, :] = raw[32:128, :]
    edge_ref[96:192, :] = raw[60 * 16 : 66 * 16, :]
    for copy in stores:
        copy.wait()


def edge_kernel(info_ref, edge_ref, halo_ref, _, out_ref, left, right, slots, sem):
    left[32:128, :] = edge_ref[0:96, :]
    right[0:96, :] = edge_ref[96:192, :]
    for j in range(16):
        rows = halo_ref[:, 128 * j : 128 * j + 128]
        left[pl.ds(j, 2, stride=16), :] = rows
        right[pl.ds(96 + j, 2, stride=16), :] = rows
    copies = []
    for i, (raw, at) in enumerate(((left, THERE_AT[0]), (right, THERE_AT[15]))):
        for cell in range(4):
            for half in range(2):
                near = [
                    raw[16 * (cell + k) + 8 * half : 16 * (cell + k) + 8 * half + 8, :] for k in range(5)
                ]
                slots[i, pl.ds(2 * cell + half, 8, stride=8), :] = upwind(near, info_ref, half)
        copies.append(pltpu.make_async_copy(slots.at[i], out_ref.at[at], sem.at[i]))
        copies[-1].start()
    for copy in copies:
        copy.wait()


def tables_kernel(
    where_ref, order_ref, kern_ref, const_ref, base_ref, ks_ref, mask_ref, rows, turned
):
    position = lax.broadcasted_iota(jnp.int32, (1, 64), 1)
    first = position < BLOCK_CELLS * where_ref[1]
    for c in range(4):
        hit = jnp.where(first & (order_ref[...] == 4 * where_ref[0] + c), STEP_SCALE, 0.0)
        mask_ref[2 * c : 2 * c + 2, :] = jnp.broadcast_to(jnp.sum(hit, axis=1, keepdims=True), (2, 128))
    base_ref[...] = const_ref[0:576, :]
    for kx in range(32):
        for ch in range(8):
            at = kx * 8 + ch
            back = ((32 - kx) % 32) * 8 + ch
            tile = kern_ref[:, at * 128 : at * 128 + 128]
            rows[pl.ds(at, KERN, stride=256), :] = tile
            turned[pl.ds(back, KERN, stride=256), :] = tile
    group = lax.broadcasted_iota(jnp.int32, (32, 128), 1) // 32

    def ordered(src, t, k8):
        g, h = k8 % 4, k8 // 4
        out = None
        for k4 in range(4):
            piece = src[pl.ds(t * 256 + 2 * k4 + h, 32, stride=8), :]
            if k4 != g:
                piece = pltpu.roll(piece, ((k4 - g) % 4) * 32, 1)
            out = piece if out is None else jnp.where(group == k4, piece, out)
        return out

    scale = 0.5 / NV**3
    for k8 in range(8):
        at = 576 if k8 == 0 else 704
        flip = const_ref[at : at + 128, :].astype(BF16)
        for t in range(KERN):
            straight = ordered(rows, t, k8)
            other = ordered(turned, t, (8 - k8) % 8)
            hi, lo = split(other)
            ks_ref[k8, t] = scale * (straight + (dot(hi, flip) + dot(lo, flip)))


def turn(k8, lane_y4):
    cvec = jnp.full((1, 128), 1.0, F32)
    svec = jnp.full((1, 128), 0.0, F32)
    for y4 in range(1, 4):
        angle = 2 * math.pi * y4 * k8 / 32
        cvec = jnp.where(lane_y4 == y4, math.cos(angle), cvec)
        svec = jnp.where(lane_y4 == y4, math.sin(angle), svec)
    return cvec, svec


ROOT = math.sqrt(0.5)
PAIRS = ((0, 4), (1, 7), (2, 6), (3, 5))


def forward8(x):
    a = [x[j] + x[j + 4] for j in range(4)]
    d = [x[j] - x[j + 4] for j in range(4)]
    even, odd = a[0] + a[2], a[1] + a[3]
    less, more = ROOT * (d[1] - d[3]), ROOT * (d[1] + d[3])
    return (
        (even + odd, even - odd),
        (d[0] + less, -d[2] - more),
        (a[0] - a[2], a[3] - a[1]),
        (d[0] - less, d[2] - more),
    )


def inverse8(r0, r4, c1, s1, c2, s2, c3, s3):
    e, o = r0 + r4, r0 - r4
    a, b, c, d = e + c2, e - c2, c1 + c3, s3 - s1
    p, q = o - s2, o + s2
    less, more = ROOT * (c1 - c3), ROOT * (s1 + s3)
    m, n = less - more, less + more
    return [a + c, p + m, b + d, q - n, a - c, p - m, b - d, q + n]


def right(base_ref, k8, inverse):
    c, s = base_ref[0:128, :], base_ref[128:256, :]
    if k8:
        cvec, svec = turn(k8, lax.broadcasted_iota(jnp.int32, (1, 128), 1) // 32)
        c, s = cvec * c - svec * s, cvec * s + svec * c
    halves = []
    for c, s in zip(split(c), split(s)):
        up, down = (s, -s) if inverse else (-s, s)
        halves.append(
            jnp.concatenate(
                [jnp.concatenate([c, up], axis=1), jnp.concatenate([down, c], axis=1)], axis=0
            )
        )
    return halves


def left_matrices(base_ref, lf_ref, li_ref):
    zero = jnp.zeros((32, 128), BF16)
    c, s = base_ref[256:288, :], base_ref[288:320, :]
    cell = (lax.broadcasted_iota(jnp.int32, (32, 128), 1) % 8) // 2
    for p in range(2):
        first, second = cell == 2 * p, cell == 2 * p + 1
        real = split(jnp.where(first, c, jnp.where(second, s, 0.0)))
        imag = split(jnp.where(first, -s, jnp.where(second, c, 0.0)))
        for half in range(2):
            re, im = real[half], imag[half]
            for kk in range(2):
                at = 128 * kk + 64 * p
                top, low = slice(at, at + 32), slice(at + 32, at + 64)
                mine, other = slice(128 * kk, 128 * kk + 128), slice(128 - 128 * kk, 256 - 128 * kk)
                lf_ref[0, half, top, mine], lf_ref[0, half, low, mine] = re, im
                lf_ref[0, half, top, other], lf_ref[0, half, low, other] = zero, zero
                lf_ref[1, half, top, 0:128], lf_ref[1, half, low, 0:128] = re, im
                lf_ref[1, half, top, 128:256] = im if kk else -im
                lf_ref[1, half, low, 128:256] = -re if kk else re
    zero = jnp.zeros((128, 128), BF16)
    c, s = base_ref[320:448, :], base_ref[448:576, :]
    cell = (lax.broadcasted_iota(jnp.int32, (128, 128), 0) % 8) // 2
    lane = lax.broadcasted_iota(jnp.int32, (128, 128), 1)
    first, second = cell == 2 * (lane // 64), cell == 2 * (lane // 64) + 1
    real = (lane // 32) % 2 == 0
    zeroth = split(jnp.where(first, jnp.where(real, c, -s), jnp.where(second, jnp.where(real, s, c), 0.0)))
    other = split(jnp.where(first, jnp.where(real, s, c), jnp.where(second, jnp.where(real, -c, s), 0.0)))
    for half in range(2):
        a, b = zeroth[half], other[half]
        up, low = slice(0, 128), slice(128, 256)
        li_ref[0, half, up, up], li_ref[0, half, up, low] = a, zero
        li_ref[0, half, low, up], li_ref[0, half, low, low] = zero, a
        li_ref[1, half, up, up], li_ref[1, half, up, low] = a, a
        li_ref[1, half, low, up], li_ref[1, half, low, low] = b, -b


def columns(g, t):
    at = 128 * (t if g == 0 else KERN + 3 * t + g - 1)
    return slice(at, at + 128)


def collide_kernel(
    x_ref, base_ref, ks_ref, mask_ref, out_ref, lf_ref, li_ref, fh, fl, y, gh, gl, spec, mh, ml, back, total
):
    left_matrices(base_ref, lf_ref, li_ref)
    for v in range(0, 16, 2):
        x = [
            jnp.concatenate(
                [x_ref[THERE_AT[v + i], 8 * ch : 8 * ch + 8, :] for i in range(2)], axis=0
            )
            for ch in range(8)
        ]
        for g, parts in enumerate(forward8(x)):
            for u, part in enumerate(parts):
                rows, lanes = slice(128 * u + 8 * v, 128 * u + 8 * v + 16), slice(128 * g, 128 * g + 128)
                fh[rows, lanes], fl[rows, lanes] = split(part)
    for i, lanes in enumerate((slice(0, 128), slice(128, 512))):
        y[:, lanes] = dot3(lf_ref[i, 0], lf_ref[i, 1], fh[:, lanes], fl[:, lanes])
    lane_y4 = lax.broadcasted_iota(jnp.int32, (1, 128), 1) // 32
    for g in range(4):
        for kk in range(2):
            k8 = PAIRS[g][kk]
            cvec, svec = turn(k8, lane_y4)
            for p in range(2):
                at = 128 * kk + 64 * p
                lanes = slice(128 * g, 128 * g + 128)
                re, im = y[at : at + 32, lanes], y[at + 32 : at + 64, lanes]
                if k8:
                    re, im = re * cvec + im * svec, im * cvec - re * svec
                rows = slice(64 * k8 + 32 * p, 64 * k8 + 32 * p + 32)
                gh[rows, 0:128], gl[rows, 0:128] = split(re)
                gh[rows, 128:256], gl[rows, 128:256] = split(im)
    spec[...] = dot3(gh[...], gl[...], *right(base_ref, 0, False))
    for g in range(4):
        for kk in range(2):
            k8 = PAIRS[g][kk]
            parts = []
            for t in range(KERN):
                ks = ks_ref[k8, t]
                ks = jnp.concatenate([ks, ks], axis=1)
                for p in range(2):
                    at = 64 * k8 + 32 * p
                    parts.append(spec[at : at + 32, :] * ks)
            hi, lo = split(jnp.concatenate(parts, axis=0))
            done = dot3(hi, lo, *right(base_ref, k8, True))
            hi, lo = split(done)
            for n in range(2 * KERN):
                t, p = n // 2, n % 2
                for ri in range(2):
                    at = 128 * kk + 64 * p + 32 * ri
                    part = (slice(32 * n, 32 * n + 32), slice(128 * ri, 128 * ri + 128))
                    mh[at : at + 32, columns(g, t)] = hi[part]
                    ml[at : at + 32, columns(g, t)] = lo[part]

    def over_x(i, lanes):
        back[:, lanes] = dot3(li_ref[i, 0], li_ref[i, 1], mh[:, lanes], ml[:, lanes])

    def values(v, t):
        parts = [
            back[128 * u + 8 * v : 128 * u + 8 * v + 8, columns(g, t)]
            for g in range(4)
            for u in range(2)
        ]
        return inverse8(*parts)

    over_x(0, slice(0, 128 * KERN))
    over_x(1, slice(columns(1, 0).start, columns(3, 1).stop))
    for v in range(16):
        for ch, (a, b) in enumerate(zip(values(v, 0), values(v, 1))):
            total[v, 8 * ch : 8 * ch + 8, :] = a * b
    over_x(1, slice(columns(1, 2).start, columns(3, 3).stop))
    for v in range(16):
        for ch, (a, b) in enumerate(zip(values(v, 2), values(v, 3))):
            total[v, 8 * ch : 8 * ch + 8, :] = total[v, 8 * ch : 8 * ch + 8, :] + a * b
    over_x(1, slice(columns(1, 4).start, columns(3, 4).stop))
    mask = mask_ref[...]
    for v in range(16):
        for ch, loss in enumerate(values(v, 4)):
            rows = slice(8 * ch, 8 * ch + 8)
            f = x_ref[THERE_AT[v], rows, :]
            out_ref[BACK_AT[v], rows, :] = f + mask * (total[v, rows, :] - f * loss)


def place_kernel(in_ref, out_ref, out, sem):
    stores = [
        pltpu.make_async_copy(out.at[pl.ds(16 * i, 16)], out_ref.at[pl.ds(16 * i, 16)], sem.at[i])
        for i in range(4)
    ]
    for tile in range(8):
        for x2 in range(2):
            for ch in range(8):
                j = 8 * x2 + ch
                for k in range(2):
                    at = BACK_AT[2 * tile + k] * SLOT + 8 * ch + x2
                    out[8 * tile + 4 * k : 8 * tile + 4 * k + 4, 128 * j : 128 * j + 128] = in_ref[
                        pl.ds(at, 4, stride=2), :
                    ]
        if tile % 2 == 1:
            stores[tile // 2].start()
    for copy in stores:
        copy.wait()


VM = pl.BlockSpec(memory_space=pltpu.VMEM)
SM = pl.BlockSpec(memory_space=pltpu.SMEM)
ANY = pl.BlockSpec(memory_space=pl.ANY)


def shape(*dims, dtype=F32):
    return jax.ShapeDtypeStruct(dims, dtype)


def params(mib):
    return pltpu.CompilerParams(vmem_limit_bytes=mib << 20)


def transport(info, dist):
    return pl.pallas_call(
        transport_kernel,
        out_shape=[shape(16, SLOT, 128), shape(192, 128)],
        in_specs=[VM, VM],
        out_specs=[ANY, VM],
        scratch_shapes=[
            pltpu.VMEM((68 * 16, 128), F32),
            pltpu.VMEM((16, SLOT, 128), F32),
            pltpu.SemaphoreType.DMA((16,)),
        ],
        compiler_params=params(8),
        cost_estimate=pl.CostEstimate(flops=4000000, bytes_accessed=1 << 20, transcendentals=0),
        name="transport",
    )(info, dist)


def edges(info, edge, halo, mine):
    return pl.pallas_call(
        edge_kernel,
        out_shape=shape(16, SLOT, 128),
        in_specs=[VM, VM, VM, ANY],
        out_specs=ANY,
        input_output_aliases={3: 0},
        scratch_shapes=[
            pltpu.VMEM((128, 128), F32),
            pltpu.VMEM((128, 128), F32),
            pltpu.VMEM((2, SLOT, 128), F32),
            pltpu.SemaphoreType.DMA((2,)),
        ],
        compiler_params=params(8),
        name="edges",
    )(info, edge, halo, mine)


def make_tables(where, order, kernels):
    rows = pltpu.VMEM((KERN * 256, 128), F32)
    return pl.pallas_call(
        tables_kernel,
        out_shape=[shape(576, 128), shape(8, KERN, 32, 128), shape(8, 128)],
        in_specs=[SM] + [VM] * 3,
        out_specs=[VM] * 3,
        scratch_shapes=[rows, rows],
        compiler_params=params(12),
        cost_estimate=pl.CostEstimate(flops=8000000, bytes_accessed=4 << 20, transcendentals=0),
        name="tables",
    )(where, order, kernels, jnp.asarray(constant_rows()))


def collide(x, tables):
    left = pltpu.VMEM((2, 2, 256, 256), BF16)
    half = pltpu.VMEM((256, 512), BF16)
    field = pltpu.VMEM((512, 256), BF16)
    wide = pltpu.VMEM((256, 2560), BF16)
    return pl.pallas_call(
        collide_kernel,
        out_shape=shape(16, SLOT, 128),
        in_specs=[VM] * 4,
        out_specs=VM,
        scratch_shapes=[
            left,
            left,
            half,
            half,
            pltpu.VMEM((256, 512), F32),
            field,
            field,
            pltpu.VMEM((512, 256), F32),
            wide,
            wide,
            pltpu.VMEM((256, 2560), F32),
            pltpu.VMEM((16, SLOT, 128), F32),
        ],
        compiler_params=pltpu.CompilerParams(
            vmem_limit_bytes=20 << 20
        ),
        name="collide",
    )(x, *tables)


def place(x):
    return pl.pallas_call(
        place_kernel,
        out_shape=shape(64, 2048),
        in_specs=[VM],
        out_specs=ANY,
        scratch_shapes=[pltpu.VMEM((64, 2048), F32), pltpu.SemaphoreType.DMA((4,))],
        compiler_params=params(8),
        name="place",
    )(x.reshape(16 * SLOT, 128))


def exchange(slots, order):
    return lax.all_to_all(
        slots, "vel", split_axis=0, concat_axis=0, tiled=True, axis_index_groups=[list(order)]
    )


def local(distribution, collision_order, collision_blocks, kernels):
    v = lax.axis_index("vel")
    rising = v >= 8
    row = lax.broadcasted_iota(jnp.int32, (24, 128), 0)
    x = (2 * v + (row >= 16)).astype(F32)
    courant = jnp.abs(COURANT_MAX * (2.0 * x - (NV - 1)) / (NV - 1))
    info = jnp.where(row < 8, jnp.where(rising, 1.0, -1.0), courant)
    pairs = []
    for s in range(16):
        for u in range(16):
            to = s + 1 if u >= 8 else s - 1
            if 0 <= to < 16:
                pairs.append((s * 16 + u, to * 16 + u))
    send = lax.dynamic_slice(distribution, (jnp.where(rising, 62, 0), 0), (2, 2048))
    mine, edge = transport(info, distribution)
    halo = lax.ppermute(send, ("space", "vel"), pairs)
    mine = edges(info, edge, halo, mine)
    where = jnp.stack([v.astype(jnp.int32), collision_blocks[0]])
    tables = make_tables(where, collision_order, kernels)
    cells = exchange(mine, THERE)
    return place(exchange(collide(cells, tables), BACK))


def solution(mesh):
    in_specs = (P("space", "vel"), P("space", None), P("space"), P())
    out_specs = P("space", "vel")
    return jax.shard_map(local, mesh=mesh, in_specs=in_specs, out_specs=out_specs, check_vma=False)
```
